256 devices in a mesh: rep: 2 (over core), dp: 128 (over x, y, z).
Axes of the slice: x: 4, y: 4, z: 8, core: 2. Of those that a mesh axis runs over, the one named last changes fastest.
Arguments:
- x: bfloat16 [256, 2048, 768], P(('rep', 'dp')), parts along dimension 0
- dy: bfloat16 [256, 2048, 768], P(('rep', 'dp')), parts along dimension 0
- wq: bfloat16 [1, 768, 768], P(None, 'dp')
- wk: bfloat16 [1, 768, 128], P(None, 'dp')
- wv: bfloat16 [1, 768, 128], P(None, 'dp')
- wo: bfloat16 [1, 768, 768], P(None, 'dp')
- w_gate: bfloat16 [1, 768, 2048], P(None, 'dp')
- w_up: bfloat16 [1, 768, 2048], P(None, 'dp')
- w_down: bfloat16 [1, 2048, 768], P(None, 'dp')
Outputs:
- output 1: bfloat16 [256, 2048, 768], P(('rep', 'dp')), parts along dimension 0
- output 2: bfloat16 [2, 768, 768], P('rep', 'dp'), parts along dimension 0
- output 3: bfloat16 [2, 768, 128], P('rep', 'dp'), parts along dimension 0
- output 4: bfloat16 [2, 768, 128], P('rep', 'dp'), parts along dimension 0
- output 5: bfloat16 [2, 768, 768], P('rep', 'dp'), parts along dimension 0
- output 6: bfloat16 [2, 768, 2048], P('rep', 'dp'), parts along dimension 0
- output 7: bfloat16 [2, 768, 2048], P('rep', 'dp'), parts along dimension 0
- output 8: bfloat16 [2, 2048, 768], P('rep', 'dp'), parts along dimension 0
There are 2 independent parts. The reference program is written for one: setup_inputs(seed, part) draws one part's arguments, and reference() takes and returns one part's arrays. A program takes and returns all parts, laid end to end along the dimension named above; an argument that names none is the same for every part.
All inputs are finite; a program needn't handle non-finite values.
Results may differ from the reference program's by a relative error of at most 0.024.
Values are sent between devices in bfloat16 or wider.
A program may use at most 768 MiB of HBM per device.

```python
import jax
import jax.numpy as jnp
from jax import lax

SEQUENCES = 128
TOKENS = 2048
D = 768
HEADS = 6
KV_HEADS = 1
HEAD = 128
FF = 2048
LAYERS = 1
THETA = 10000
NAMES = ("wq", "wk", "wv", "wo", "w_gate", "w_up", "w_down")
SHAPES = {
    "wq": (LAYERS, D, HEADS * HEAD),
    "wk": (LAYERS, D, KV_HEADS * HEAD),
    "wv": (LAYERS, D, KV_HEADS * HEAD),
    "wo": (LAYERS, HEADS * HEAD, D),
    "w_gate": (LAYERS, D, FF),
    "w_up": (LAYERS, D, FF),
    "w_down": (LAYERS, FF, D),
}


def bump(key, n, height):
    away = (jnp.arange(n, dtype=jnp.int32) - jax.random.randint(key, (), 0, n, jnp.int32)) % n
    return jnp.where(away < n // 8, height, 1.0)


def together(key, own, strength):
    shared = jax.random.normal(key, own.shape[1:], jnp.float32)
    return (own + strength * shared) * lax.rsqrt(1 + strength * strength)


def setup_inputs(seed: int = 0, part: int = 0) -> dict:
    kx, kdy, ka, kb, kz, kf, kh, kl, *keys = jax.random.split(jax.random.key(seed), 8 + 3 * len(NAMES))
    kx, kdy, ka, kb = (jax.random.fold_in(k, part) for k in (kx, kdy, ka, kb))
    kw, km, kv = (keys[i::3] for i in range(3))
    shape = (SEQUENCES, TOKENS, D)
    much_x, much_dy = jax.random.uniform(kz, (2,), jnp.float32, 0.0, 1.0)
    loud = 2.0 ** jax.random.uniform(jax.random.fold_in(kz, 1), (), jnp.float32, -1.0, 2.0)
    layers = 2.0 ** jax.random.uniform(kl, (LAYERS, 1, 1), jnp.float32, -1.0, 1.0)
    times = {"wq": 1.0, "wk": 1.0, "wv": 2.0, "wo": layers, "w_gate": 1.0, "w_up": bump(kh, FF, 4.0), "w_down": layers}
    x = together(ka, jax.random.normal(kx, shape, jnp.float32), much_x) * bump(kf, D, 4.0)
    dy = together(kb, jax.random.normal(kdy, shape, jnp.float32), much_dy)
    drawn = {"x": x.astype(jnp.bfloat16), "dy": (loud * dy * (SEQUENCES * TOKENS) ** -0.5).astype(jnp.bfloat16)}
    for key, name in zip(kw, NAMES, strict=True):
        drawn[name] = (jax.random.normal(key, SHAPES[name], jnp.float32) * SHAPES[name][1] ** -0.5 * times[name]).astype(jnp.bfloat16)
    return drawn


def matmul(a, w):
    return jnp.dot(a, w, preferred_element_type=jnp.float32).astype(jnp.bfloat16)


def normed(h):
    wide = h.astype(jnp.float32)
    scale = lax.rsqrt(jnp.mean(wide**2, -1, keepdims=True) + 1e-6)
    return (wide * scale).astype(jnp.bfloat16)


def turned(t, theta):
    half = t.shape[-1] // 2
    angle = jnp.arange(t.shape[0], dtype=jnp.float32)[:, None] * theta ** (-jnp.arange(half, dtype=jnp.float32) / half)
    cos, sin = jnp.cos(angle)[:, None], jnp.sin(angle)[:, None]
    a, b = t[..., :half].astype(jnp.float32), t[..., half:].astype(jnp.float32)
    return jnp.concatenate([a * cos - b * sin, b * cos + a * sin], -1).astype(jnp.bfloat16)


def seen_by(q, k, v):
    tokens, kv = q.shape[0], k.shape[1]
    q = q.reshape(tokens, kv, -1, q.shape[-1])
    scores = jnp.einsum("tgsd,ugd->gstu", q.astype(jnp.float32), k.astype(jnp.float32)) * q.shape[-1] ** -0.5
    place = jnp.arange(tokens)
    weights = jax.nn.softmax(jnp.where(place[:, None] >= place, scores, -jnp.inf), -1).astype(jnp.bfloat16)
    return jnp.einsum("gstu,ugd->tgsd", weights.astype(jnp.float32), v.astype(jnp.float32)).astype(jnp.bfloat16).reshape(tokens, -1)


def layer(h, w):
    a = normed(h)
    q, k = (turned(matmul(a, w[name]).reshape(h.shape[0], -1, HEAD), THETA) for name in ("wq", "wk"))
    h = h + matmul(seen_by(q, k, matmul(a, w["wv"]).reshape(h.shape[0], -1, HEAD)), w["wo"])
    b = normed(h)
    gate = jnp.dot(b, w["w_gate"], preferred_element_type=jnp.float32)
    up = jnp.dot(b, w["w_up"], preferred_element_type=jnp.float32)
    return h + matmul((jax.nn.silu(gate) * up).astype(jnp.bfloat16), w["w_down"])


def stack(weights, h):
    return lax.scan(lambda h, w: (layer(h, w), None), h, weights)[0]


def reference(x, dy, wq, wk, wv, wo, w_gate, w_up, w_down):
    weights = dict(zip(NAMES, (wq, wk, wv, wo, w_gate, w_up, w_down), strict=True))

    def take(so_far, sequence):
        h, by_y = sequence
        _, back = jax.vjp(stack, weights, h)
        by_weights, by_h = back(by_y)
        return jax.tree.map(lambda total, term: total + term.astype(jnp.float32), so_far, by_weights), by_h

    none_yet = {name: jnp.zeros(w.shape, jnp.float32) for name, w in weights.items()}
    by_weights, by_x = lax.scan(take, none_yet, (x, dy))
    return (by_x, *(by_weights[name].astype(jnp.bfloat16) for name in NAMES))
```

```python
import functools

import jax
import jax.numpy as jnp
import numpy as np
from jax import lax
from jax.experimental import pallas as pl
from jax.experimental.pallas import tpu as pltpu
from jax.sharding import PartitionSpec as P

NEG = -1e30
HIDDEN = 2 * NEG
LOG2E = 1.4426950408889634
TOKENS, WIDTH, HEADS, HEAD, FF, THETA = 2048, 768, 6, 128, 2048, 10000
QKV, KEYS = 1024, HEADS * HEAD
LOW, WIDE = jnp.bfloat16, jnp.float32
TB = 512
SUB = 256
SCALE = HEAD**-0.5
E = SCALE * LOG2E
BK, STRIP = 512, 512
BQ = 256
CHUNK = 256
XS, YS, ZS = 4, 4, 8
FOUR = (1, 2, 3)
EIGHT = tuple(range(1, ZS))
ROWS = WIDTH // (XS * YS)
EACH = ROWS // ZS
TILE = 16
DOWN = FF // (XS * YS)
ALL = slice(None)
VMEM, DMA = pltpu.VMEM, pltpu.SemaphoreType.DMA


def _dot(a, b, ca, cb):
    return lax.dot_general(a, b, (((ca,), (cb,)), ((), ())), preferred_element_type=WIDE)


def mm(a, b):
    return _dot(a, b, 1, 0)


def mm_t(a, b):
    return _dot(a, b, 1, 1)


def t_mm(a, b):
    return _dot(a, b, 0, 0)


def low(*shape):
    return jax.ShapeDtypeStruct(shape, LOW)


def wide(*shape):
    return jax.ShapeDtypeStruct(shape, WIDE)


def many(n, size):
    return pl.multiple_of(n * size, size)


def tile(n, size=TILE):
    return pl.ds(many(n, size), size)


def block(*shape, at=lambda i: i, dim=0):
    return pl.BlockSpec(shape, lambda i: tuple(at(i) if n == dim else 0 for n in range(len(shape))))


def whole(*shape):
    return pl.BlockSpec(shape, lambda i: (0,) * len(shape), pipeline_mode=pl.Buffered(1))


def call(kernel, name, steps, ins, outs, scratch, flops, number=None):
    more = {} if number is None else {"collective_id": number, "has_side_effects": True}
    moved = sum(a.size * a.dtype.itemsize for a, _ in (*ins, *outs))
    return pl.pallas_call(
        kernel,
        name=name,
        grid=(steps,),
        in_specs=[s for _, s in ins],
        out_specs=[s for _, s in outs],
        out_shape=[a for a, _ in outs],
        scratch_shapes=scratch,
        compiler_params=pltpu.CompilerParams(dimension_semantics=("arbitrary",), vmem_limit_bytes=67_000_000, **more),
        cost_estimate=pl.CostEstimate(flops=flops, bytes_accessed=moved, transcendentals=0),
    )(*[a for a, _ in ins])


def on(n):
    return pl.when(pl.program_id(0) == n)


def always(f):
    f()


MESH = pl.DeviceIdType.MESH


def place():
    me = lax.axis_index("dp")
    return lax.axis_index("rep"), me // (YS * ZS), (me // ZS) % YS, me % ZS


def at(x, y, z):
    return {"dp": (x * YS + y) * ZS + z}


def meet(sibling):
    c, x, y, z = place()
    devices = [at(x, y, (z + d) % ZS) for d in EIGHT] + [at(x, (y + d) % YS, z) for d in FOUR] + [at((x + d) % XS, y, z) for d in FOUR]
    devices += [{"rep": 1 - c}] if sibling else []
    barrier = pltpu.get_barrier_semaphore()
    for device in devices:
        pl.semaphore_signal(barrier, inc=1, device_id=device, device_id_type=MESH)
    pl.semaphore_wait(barrier, len(devices))


def remote(src, dst, sems, at_sem, device):
    return pltpu.make_async_remote_copy(src_ref=src, dst_ref=dst, send_sem=sems[0].at[at_sem], recv_sem=sems[1].at[at_sem], device_id=device, device_id_type=MESH)


def start(copies):
    for copy in copies:
        copy.start()


def arrive(copies):
    for copy in copies:
        copy.wait_recv()


def leave(copies):
    for copy in copies:
        copy.wait_send()


class Gather:
    def __init__(self, number, out, buf, cut, sems):
        self.number, self.out, self.buf, self.sems = number, out, buf, sems
        self.c, self.x, self.y, self.z = place()
        self.half = out.shape[3] // 2
        self.a, self.b = (pl.ds(pl.multiple_of(self.c * self.half + s, HEAD), n) for s, n in ((0, cut), (cut, self.half - cut)))
        self.other = {"rep": 1 - self.c}

    def along_z(self):
        if self.buf is None:
            own = self.out.at[self.x, self.y, tile(self.z), pl.ds(pl.multiple_of(self.c * self.half, HEAD), self.half)]
        else:
            own = self.buf.at[self.z]
        return [remote(own, own, self.sems[0], (self.number, d - 1), at(self.x, self.y, (self.z + d) % ZS)) for d in EIGHT]

    def assemble(self, tmp):
        half = self.half
        for j in range(ZS):
            tmp[EACH * j : EACH * j + EACH, :half] = self.buf[j, :EACH, :].astype(WIDE)
        for n in range(2):
            @pl.when(self.c == n)
            def _():
                self.out[self.x, self.y, :, n * half : n * half + half] = tmp[:, :half].astype(LOW)

    def to_x(self, ref, sems, at_sem, ds=FOUR):
        return [remote(ref, ref, sems, (self.number, *at_sem, d), at((self.x + d) % XS, self.y, self.z)) for d in ds]

    def to_y(self, ref, sems, at_sem, ds=FOUR):
        return [remote(ref, ref, sems, (self.number, *at_sem, d), at(self.x, (self.y + d) % YS, self.z)) for d in ds]

    def second_a(self):
        return self.to_y(self.out.at[self.x, self.y, :, self.a], self.sems[1], (0,))

    def second_b(self):
        return self.to_x(self.out.at[self.x, self.y, :, self.b], self.sems[1], (1,))

    def third_a(self, ds=FOUR):
        return self.to_x(self.out.at[self.x, :, :, self.a], self.sems[2], (0,), ds)

    def third_b(self, ds=FOUR):
        return self.to_y(self.out.at[:, self.y, :, self.b], self.sems[2], (1,), ds)

    def cross_a(self, d):
        got = self.out.at[(self.x - d + XS) % XS, :, :, self.a]
        return [remote(got, got, self.sems[3], (self.number, 0, d), self.other)]

    def cross_b(self, d):
        got = self.out.at[:, (self.y - d + YS) % YS, :, self.b]
        return [remote(got, got, self.sems[3], (self.number, 1, d), self.other)]

    def spread(self):
        arrive(self.second_a())
        start(self.third_a())
        arrive(self.second_b())
        start(self.third_b() + self.cross_a(0) + self.cross_b(0))

    def cross(self):
        for d in (1, 3, 2):
            arrive(self.third_a((d,)))
            start(self.cross_a(d))
            arrive(self.third_b((d,)))
            start(self.cross_b(d))

    def crossed(self):
        for d in range(XS):
            arrive(self.cross_a(d) + self.cross_b(d))

    def finish(self):
        leave(self.along_z() + self.second_a() + self.second_b() + self.third_a() + self.third_b())
        for d in range(XS):
            leave(self.cross_a(d) + self.cross_b(d))


class Scatter:
    @staticmethod
    def scratch(chunks, rows, cols):
        return [VMEM((3, chunks, 4, rows, cols), LOW), VMEM((4, chunks, rows, cols), LOW), VMEM((3, chunks, rows, cols), LOW)]

    def __init__(self, number, x_first, term, own, bufs, sems):
        self.number, self.term, self.own, self.sems = number, term, own, sems
        self.got, self.part, self.got2 = bufs
        c, x, y, self.z = place()
        self.p, self.q = (x, y) if x_first else (y, x)
        self.chip = (lambda p, q, z: at(p, q, z)) if x_first else (lambda p, q, z: at(q, p, z))
        self.chunks, self.rows, cols = own.shape
        self.step = {ROWS: ROWS, DOWN: DOWN // 2}[self.rows] if cols <= CHUNK else TILE

    def first(self, s):
        return [remote(self.term(s, (self.p + d) % 4), self.got.at[d - 1, s], self.sems[0], (self.number, d), self.chip((self.p + d) % 4, self.q, self.z)) for d in FOUR]

    def first_all(self):
        return [remote(self.got.at[d - 1], self.got.at[d - 1], self.sems[0], (self.number, d), self.chip((self.p + d) % 4, self.q, self.z)) for d in FOUR]

    def second(self):
        return [remote(self.part.at[(self.q + d) % 4], self.got2.at[d - 1], self.sems[1], (self.number, d), self.chip(self.p, (self.q + d) % 4, self.z)) for d in FOUR]

    def add_first(self):
        arrive(self.first_all())
        per = self.rows // self.step

        def total(s, b, r):
            total = self.term(s, self.p)[b, r, :].astype(WIDE)
            for d in FOUR:
                total += self.got[d - 1, s, b, r, :].astype(WIDE)
            return total

        def add(k, _):
            s, b, r = k // (3 * per), (self.q + 1 + k // per % 3) % 4, tile(k % per, self.step)
            self.part[b, s, r, :] = total(s, b, r).astype(LOW)

        lax.fori_loop(0, self.chunks * 3 * per, add, None, unroll=2)
        start(self.second())

        def keep(k, _):
            s, r = k // per, tile(k % per, self.step)
            self.own[s, r, :] = total(s, self.q, r)

        lax.fori_loop(0, self.chunks * per, keep, None)

    def add_second(self):
        arrive(self.second())
        per = self.rows // self.step

        def add(k, _):
            s, r = k // per, tile(k % per, self.step)
            total = self.own[s, r, :]
            for d in FOUR:
                total += self.got2[d - 1, s, r, :].astype(WIDE)
            self.own[s, r, :] = total

        lax.fori_loop(0, self.chunks * per, add, None)

    def finish(self):
        leave(self.first_all() + self.second())


class Last:
    @staticmethod
    def scratch(chunks, rows, cols):
        each = max(rows // ZS, 8)
        return [VMEM((ZS, chunks, each, cols), LOW), VMEM((ZS - 1, chunks, each, cols), LOW), VMEM((chunks, each, cols), WIDE)]

    def __init__(self, number, sums, bufs, sems):
        self.number, self.sums, self.sems = number, sums, sems
        self.packed, self.got, self.own = bufs
        self.chunks, rows, _ = sums.shape
        self.each = rows // ZS
        c, self.x, self.y, self.z = place()

    def clear(self):
        if self.each < 8:
            self.packed[:] = jnp.zeros_like(self.packed)

    def copies(self):
        return [remote(self.packed.at[(self.z + d) % ZS], self.got.at[d - 1], self.sems, (self.number, d - 1), at(self.x, self.y, (self.z + d) % ZS)) for d in EIGHT]

    def send(self):
        each = self.each

        def pack(s, _):
            for j in range(ZS):
                self.packed[j, s, :each, :] = self.sums[s, j * each : j * each + each, :].astype(LOW)

        lax.fori_loop(0, self.chunks, pack, None)
        start(self.copies())
        for j in range(ZS):
            @pl.when(self.z == j)
            def _():
                for s in range(self.chunks):
                    self.own[s, :each, :] = self.sums[s, j * each : j * each + each, :]

    def receive(self, store):
        arrive(self.copies())
        for s in range(self.chunks):
            total = self.own[s, : self.each, :]
            for d in EIGHT:
                total += self.got[d - 1, s, : self.each, :].astype(WIDE)
            store(s, total.astype(LOW))
        leave(self.copies())


class ScatterZ:
    @staticmethod
    def scratch(cols):
        return [VMEM((ZS - 1, XS, YS, TILE, cols), LOW), VMEM((XS, YS, TILE, cols), LOW), VMEM((3, YS, TILE, cols), LOW)]

    def __init__(self, terms, own, bufs, sems):
        self.terms, self.own, self.sems = terms, own, sems
        self.got, self.part, self.got2 = bufs
        c, self.x, self.y, self.z = place()
        self.cols = pl.ds(0, self.got.shape[4])

    def first(self, s):
        x, y = s // 2, pl.ds(s % 2 * 2, 2)
        return [remote(self.terms.at[x, y, tile((self.z + d) % ZS), self.cols], self.got.at[d - 1, x, y], self.sems[0], d - 1, at(self.x, self.y, (self.z + d) % ZS)) for d in EIGHT]

    def first_all(self):
        return [remote(self.got.at[d - 1], self.got.at[d - 1], self.sems[0], d - 1, at(self.x, self.y, (self.z + d) % ZS)) for d in EIGHT]

    def second(self):
        return [remote(self.part.at[(self.x + d) % XS], self.got2.at[d - 1], self.sems[1], d, at((self.x + d) % XS, self.y, self.z)) for d in FOUR]

    def add_first(self):
        arrive(self.first_all())

        def total(x, y):
            total = self.terms[x, y, tile(self.z), self.cols].astype(WIDE)
            for d in EIGHT:
                total += self.got[d - 1, x, y].astype(WIDE)
            return total

        def add(k, _):
            x, y = (self.x + 1 + k // YS) % XS, k % YS
            self.part[x, y] = total(x, y).astype(LOW)

        lax.fori_loop(0, len(FOUR) * YS, add, None, unroll=2)
        start(self.second())

        def keep(y, _):
            self.own[y] = total(self.x, y)

        lax.fori_loop(0, YS, keep, None)

    def add_second(self):
        arrive(self.second())

        def add(y, _):
            total = self.own[y]
            for d in FOUR:
                total += self.got2[d - 1, y].astype(WIDE)
            self.own[y] = total

        lax.fori_loop(0, YS, add, None)

    def finish(self):
        leave(self.first_all() + self.second())


class LastY:
    @staticmethod
    def scratch(cols):
        return [VMEM((YS, TILE, cols), LOW), VMEM((3, TILE, cols), LOW)]

    def __init__(self, sums, bufs, sems):
        self.sums, self.sems = sums, sems
        self.packed, self.got = bufs
        c, self.x, self.y, self.z = place()

    def copies(self):
        return [remote(self.packed.at[(self.y + d) % YS], self.got.at[d - 1], self.sems, d, at(self.x, (self.y + d) % YS, self.z)) for d in FOUR]

    def send(self):
        self.packed[:] = self.sums[:].astype(LOW)
        start(self.copies())

    def receive(self, store):
        arrive(self.copies())
        total = self.sums[self.y]
        for d in FOUR:
            total += self.got[d - 1].astype(WIDE)
        store(total.astype(LOW))
        leave(self.copies())


def pairs(*shapes):
    return [DMA(s) for s in shapes for _ in range(2)]


def paired(refs):
    return [refs[n : n + 2] for n in range(0, len(refs), 2)]


def tables():
    rate = float(THETA) ** (-np.arange(HEAD // 2, dtype=np.float64) / (HEAD // 2))
    rate = np.concatenate([rate, rate])
    near, far = (np.arange(0, n, s)[:, None] * rate for n, s in ((SUB, 1), (TOKENS, SUB)))
    arrays = [jnp.asarray(f(t).reshape(s), WIDE) for t, s in ((near, near.shape), (far, (TOKENS // SUB, 1, HEAD))) for f in (np.cos, np.sin)]
    return [(a, whole(*a.shape)) for a in arrays]


def angles(near_cos, near_sin, far_cos, far_sin, n):
    nc, ns, fc, fs = near_cos[:], near_sin[:], far_cos[n], far_sin[n]
    sign = jnp.where(lax.broadcasted_iota(jnp.int32, (1, HEAD), 1) < HEAD // 2, -1.0, 1.0)
    return fc * nc - fs * ns, (fs * nc + fc * ns) * sign


def scaled(h):
    h = h.astype(WIDE)
    scale = lax.rsqrt(jnp.mean(h * h, -1, keepdims=True) + 1e-6)
    return h, scale, (h * scale).astype(LOW)


def unscaled(by, h, scale):
    by = by.astype(LOW).astype(WIDE)
    return (by * scale - h * (scale * scale * scale * jnp.mean(by * h, -1, keepdims=True))).astype(LOW).astype(WIDE)


def front_kernel(x, wq, wk, wv, wo, wg, wu, wd, nc, ns, fc, fs, q, k, v, o, ot, lse, q_out, o_out, g_out, d_out,
                 q_w, o_w, g_w, d_w, q_z, o_z, g_z, tmp, k_s, v_s, top_s, mix_s, gap_s, done, *sems):
    i = pl.program_id(0)
    cols = HEADS * TB
    strips = range(0, cols, STRIP)
    sems = paired(sems)
    written = [pltpu.make_async_copy(src, dst, done.at[n]) for n, (src, dst) in enumerate(((q_w, q_out), (o_w, o_out), (g_w, g_out), (d_w, d_out)))]
    proj, out, gate, down = items = [Gather(n, *args, sems) for n, args in enumerate(((q_w, q_z, 256), (o_w, o_z, 256), (g_w, g_z, FF // 2), (d_w, None, 128)))]

    @on(0)
    def _():
        c, x_, y_, z_ = place()
        mine = pl.ds(0, EACH)

        @pl.when(c == 0)
        def _():
            q_z[z_, mine, :] = wq[0, :, : QKV // 2]
            g_z[z_, mine, :] = wg[0]
            o_z[z_, mine, :] = wo[0, :, : WIDTH // 2]

        @pl.when(c == 1)
        def _():
            q_z[z_, mine, : KEYS - QKV // 2] = wq[0, :, QKV // 2 :]
            q_z[z_, mine, KEYS - QKV // 2 : KEYS - QKV // 2 + HEAD] = wk[0]
            q_z[z_, mine, KEYS - QKV // 2 + HEAD :] = wv[0]
            g_z[z_, mine, :] = wu[0]
            o_z[z_, mine, :] = wo[0, :, WIDTH // 2 :]

        for buf in (q_z, o_z, g_z):
            buf[z_, EACH:, :] = jnp.zeros((buf.shape[1] - EACH, buf.shape[2]), LOW)
        for n in range(2):
            @pl.when(c == n)
            def _():
                d_w[x_, y_, tile(z_), n * down.half : n * down.half + down.half] = wd[0, :, n * down.half : n * down.half + down.half]
        gap_s[:] = lax.broadcasted_iota(jnp.int32, (BK, STRIP), 1) - lax.broadcasted_iota(jnp.int32, (BK, STRIP), 0)
        meet(True)
        rest = (gate, out, down)
        for item in (proj, *rest):
            start(item.along_z())
        arrive(proj.along_z())
        proj.assemble(tmp)
        start(proj.second_a() + proj.second_b())
        proj.spread()
        for item in rest:
            arrive(item.along_z())
            if item.buf is not None:
                item.assemble(tmp)
            start(item.second_a() + item.second_b())
        proj.cross()
        proj.crossed()
        start(written[:1])

    a = scaled(x[:])[2]
    made = mm(a, q_w[:].reshape(WIDTH, QKV))
    mine = tile(i, TB)
    for n in range(TB // SUB):
        cos, sin = angles(nc, ns, fc, fs, i * (TB // SUB) + n)
        r = slice(n * SUB, n * SUB + SUB)
        for h in range(HEADS + 1):
            t = made[r, h * HEAD : h * HEAD + HEAD].astype(LOW).astype(WIDE)
            t = (t * cos + pltpu.roll(t, HEAD // 2, 1) * sin).astype(LOW)
            if h < HEADS:
                q[h, r, :] = t
            else:
                k[r, :] = t
    v[:] = made[:, KEYS + HEAD :].astype(LOW)
    k_s[mine, :] = k[:]
    v_s[mine, :] = v[:]

    @on(0)
    def _():
        gate.spread()

    top_s[:] = jnp.full((1, cols), NEG, WIDE)
    mix_s[:] = jnp.zeros((HEAD + 8, cols), WIDE)
    ones = jnp.ones((8, BK), LOW)

    def keys(j, masked):
        here = tile(j, BK)
        scores = [mm_t(k_s[here, :], q[:].reshape(cols, HEAD)[s : s + STRIP, :]) for s in strips]
        ok = gap_s[:] >= 0 if masked else None
        weights, keeps = [], []
        for s, score in zip(strips, scores):
            if masked:
                score = jnp.where(ok, score, HIDDEN)
            old = top_s[:, s : s + STRIP]
            top = jnp.maximum(old, score.max(axis=0, keepdims=True))
            top_s[:, s : s + STRIP] = top
            weights.append(jnp.exp2((score - top) * E).astype(LOW))
            keeps.append(jnp.exp2((old - top) * E))
        values = jnp.concatenate([v_s[here, :].T, ones], axis=0)
        for s, p, keep in zip(strips, weights, keeps):
            mix_s[:, s : s + STRIP] = mix_s[:, s : s + STRIP] * keep + mm(values, p)

    lax.fori_loop(0, i, lambda j, _: keys(j, False), None)

    @on(3)
    def _():
        gate.crossed()
        start(written[2:3])
        out.cross()
        down.cross()

    keys(i, True)
    total = mix_s[HEAD : HEAD + 1, :]
    result = mix_s[:HEAD, :] * (1 / total)
    lses = top_s[:] * SCALE + jnp.log(total)
    for h in range(HEADS):
        piece = result[:, h * TB : h * TB + TB].astype(LOW)
        ot[h] = piece
        o[h] = piece.T
        lse[h : h + 1, :] = lses[:, h * TB : h * TB + TB]

    @on(0)
    def _():
        out.spread()
        down.spread()

    @on(2)
    def _():
        gate.cross()

    @on(3)
    def _():
        out.crossed()
        down.crossed()
        start(written[1::2])
        for item in items:
            item.finish()
        for copy in written:
            copy.wait()


def front(x, weights):
    heads = (HEADS, TB, HEAD)
    matrices = [(XS, YS, ROWS, QKV), (XS, YS, ROWS, WIDTH), (XS, YS, ROWS, 2 * FF), (XS, YS, DOWN, WIDTH)]
    return call(
        front_kernel, "front", TOKENS // TB,
        [(x, block(TB, WIDTH)), *[(w, whole(*w.shape)) for w in weights], *tables()],
        [(low(HEADS, TOKENS, HEAD), block(*heads, dim=1)), (low(TOKENS, HEAD), block(TB, HEAD)), (low(TOKENS, HEAD), block(TB, HEAD)),
         (low(HEADS, TOKENS, HEAD), block(*heads, dim=1)), (low(HEADS, HEAD, TOKENS), block(HEADS, HEAD, TB, dim=2)), (wide(HEADS, TOKENS), block(HEADS, TB, dim=1)),
         *[(low(*s), pl.BlockSpec(memory_space=pl.ANY)) for s in matrices]],
        [VMEM(s, LOW) for s in matrices]
        + [VMEM((ZS, 8, n), LOW) for n in (QKV // 2, WIDTH // 2, FF)]
        + [VMEM((ROWS, FF), WIDE), VMEM((TOKENS, HEAD), LOW), VMEM((TOKENS, HEAD), LOW), VMEM((1, HEADS * TB), WIDE), VMEM((HEAD + 8, HEADS * TB), WIDE),
           VMEM((BK, STRIP), jnp.int32), DMA((4,))]
        + pairs((4, 7), (4, 2, 4), (4, 2, 4), (4, 2, 4)),
        2 * TOKENS * (WIDTH * QKV + HEADS * TOKENS * HEAD), 0)


def mlp_kernel(x, dy, o, ot, wo, gu, wd, act, by_gate, by_up, bt, by_h, by_o, delta, dwo, dwo_s):
    i = pl.program_id(0)
    heads = jnp.concatenate([o[h] for h in range(HEADS)], axis=1)
    h, scale, b = scaled((x[:].astype(WIDE) + mm(heads, wo[:]).astype(LOW).astype(WIDE)).astype(LOW))
    bt[:] = b.T
    dy_b = dy[:]
    step = 512
    for s in range(0, FF, step):
        f = slice(s, s + step)
        g = mm(b, gu[:, f])
        u = mm(b, gu[:, FF + s : FF + s + step])
        by = mm_t(dy_b, wd[f, :]).astype(LOW).astype(WIDE)
        sig = 0.5 * jnp.tanh(0.5 * g) + 0.5
        silu = g * sig
        act[:, f] = (silu * u).astype(LOW)
        by_up[:, f] = (by * silu).astype(LOW)
        by_gate[:, f] = (by * u * (sig + silu * (1.0 - sig))).astype(LOW)
    by_b = mm_t(by_gate[:], gu[:, :FF]) + mm_t(by_up[:], gu[:, FF:])
    dh = (dy_b.astype(WIDE) + unscaled(by_b, h, scale)).astype(LOW)
    by_h[:] = dh
    do = mm_t(dh, wo[:]).astype(LOW)
    for n in range(HEADS):
        piece = do[:, n * HEAD : n * HEAD + HEAD]
        by_o[n] = piece
        delta[n : n + 1, :] = (piece.astype(WIDE) * o[n].astype(WIDE)).T.sum(axis=0, keepdims=True)
    term = mm(ot[:].reshape(KEYS, TB), dh)
    last = pl.num_programs(0) - 1

    @on(0)
    def _():
        dwo_s[:] = term

    @pl.when((i > 0) & (i < last))
    def _():
        dwo_s[:] += term

    @on(last)
    def _():
        dwo[:] = (dwo_s[:] + term).astype(LOW)


def mlp(x, dy, o, ot, wo, gu, wd):
    rows, ff, heads = block(TB, WIDTH), block(TB, FF), block(HEADS, TB, HEAD, dim=1)
    return call(
        mlp_kernel, "mlp", TOKENS // TB,
        [(x, rows), (dy, rows), (o, heads), (ot, block(HEADS, HEAD, TB, dim=2)), *[(w, whole(*w.shape)) for w in (wo, gu, wd)]],
        [*[(low(TOKENS, FF), ff)] * 3, (low(WIDTH, TOKENS), block(WIDTH, TB, dim=1)), (low(TOKENS, WIDTH), rows), (low(HEADS, TOKENS, HEAD), heads),
         (wide(HEADS, TOKENS), block(HEADS, TB, dim=1)), (low(KEYS, WIDTH), whole(KEYS, WIDTH))],
        [VMEM((KEYS, WIDTH), WIDE)],
        2 * TOKENS * WIDTH * (3 * WIDTH + 5 * FF))


CHUNKS = FF // CHUNK
BY_Z = 512


def back_kernel(bt, dy, act, by_gate, by_up, dwo, q, k, v, do, lse, delta, dq, dk, dv, sum_o, sum_g, sum_u, sum_d, sum_z,
                dg_s, du_s, dd_s, dq_s, dk_s, dv_s, gap_s, *rest):
    i = pl.program_id(0)
    cols = HEADS * BQ
    strips = range(0, cols, STRIP)
    sems = paired(rest[15:])
    more = slice(BY_Z, WIDTH)
    of = lambda n: rest[3 * n : 3 * n + 3]
    gate = Scatter(0, True, lambda s, to: dg_s.at[s, to], sum_g, of(0), sems)
    up = Scatter(1, False, lambda s, to: du_s.at[s, :, to], sum_u, of(1), sems)
    out = Scatter(2, True, lambda s, to: dwo.at[to], sum_o, of(2), sems)
    down = Scatter(3, False, lambda s, to: dd_s.at[:, to, :, more], sum_d, of(3), sems)
    down_z = ScatterZ(dd_s, sum_z, of(4), sems[2:])

    @on(0)
    def _():
        place_ = lax.broadcasted_iota(jnp.int32, (BK, STRIP), 1)
        gap_s[:] = jnp.where(place_ >= BQ, place_ - BQ, place_) - lax.broadcasted_iota(jnp.int32, (BK, STRIP), 0)
        dk_s[:] = jnp.zeros_like(dk_s)
        dv_s[:] = jnp.zeros_like(dv_s)
        meet(False)
        start(out.first(0))

    @pl.when(i < CHUNKS)
    def _():
        dd_s[i // 2, pl.ds(i % 2 * 2, 2)] = t_mm(act[:], dy[:]).astype(LOW).reshape(2, DOWN, WIDTH)
        start(down_z.first(i))
        dg_s[i] = mm(bt[:], by_gate[:]).astype(LOW).reshape(XS, YS, ROWS, CHUNK)
        start(gate.first(i))
        du_s[i] = mm(bt[:], by_up[:]).astype(LOW).reshape(XS, YS, ROWS, CHUNK)
        start(up.first(i))

    @on(CHUNKS - 1)
    def _():
        start(down.first(0))

    @on(CHUNKS + 5)
    def _():
        for item in (out, gate, up, down, down_z):
            item.add_first()

    @pl.when(i >= CHUNKS)
    def _():
        iq = i - CHUNKS
        dq_s[:] = jnp.zeros_like(dq_s)
        lses = jnp.concatenate([lse[h : h + 1, :] for h in range(HEADS)], axis=1) * LOG2E
        deltas = jnp.concatenate([delta[h : h + 1, :] for h in range(HEADS)], axis=1)

        def keys(j, masked):
            here = tile(j, BK)
            qs = [q[:].reshape(cols, HEAD)[s : s + STRIP, :] for s in strips]
            dos = [do[:].reshape(cols, HEAD)[s : s + STRIP, :] for s in strips]
            scores = [mm_t(k[here, :], t) for t in qs]
            dps = [mm_t(v[here, :], t) for t in dos]
            kt = k[here, :].T
            ok = gap_s[:] >= j * BK - iq * BQ if masked else None
            for n, s in enumerate(strips):
                p = jnp.exp2(scores[n] * E - lses[:, s : s + STRIP])
                if masked:
                    p = jnp.where(ok, p, 0.0)
                ds = (p * (dps[n] - deltas[:, s : s + STRIP])).astype(LOW)
                dv_s[here, :] += mm(p.astype(LOW), dos[n])
                dk_s[here, :] += mm(ds, qs[n])
                dq_s[:, s : s + STRIP] += mm(kt, ds)

        full = iq * BQ // BK
        lax.fori_loop(0, full, lambda j, _: keys(j, False), None)
        keys(full, True)
        for h in range(HEADS):
            dq[h] = (dq_s[:, h * BQ : h * BQ + BQ] * SCALE).T.astype(LOW)

    @on(CHUNKS + TOKENS // BQ - 1)
    def _():
        dk[:] = (dk_s[:] * SCALE).astype(LOW)
        dv[:] = dv_s[:].astype(LOW)

        for item in (down_z, out, gate, up, down):
            item.add_second()
            item.finish()


def back(bt, dy, act, by_gate, by_up, dwo, q, k, v, do, lse, delta):
    early, late = (lambda i: jnp.minimum(i, CHUNKS - 1)), (lambda i: jnp.maximum(i - CHUNKS, 0))
    cols = block(TOKENS, CHUNK, at=early, dim=1)
    heads, stats = block(HEADS, BQ, HEAD, at=late, dim=1), block(HEADS, BQ, at=late, dim=1)
    keys = whole(TOKENS, HEAD)
    sums = [(1, ROWS, WIDTH), (CHUNKS, ROWS, CHUNK), (CHUNKS, ROWS, CHUNK), (1, DOWN, WIDTH - BY_Z), (YS, TILE, BY_Z)]
    return call(
        back_kernel, "back", CHUNKS + TOKENS // BQ,
        [(bt, whole(WIDTH, TOKENS)), (dy, whole(TOKENS, WIDTH)), (act, cols), (by_gate, cols), (by_up, cols), (dwo, whole(*dwo.shape)),
         (q, heads), (k, keys), (v, keys), (do, heads), (lse, stats), (delta, stats)],
        [(low(HEADS, TOKENS, HEAD), heads), (low(TOKENS, HEAD), keys), (low(TOKENS, HEAD), keys), *[(wide(*s), whole(*s)) for s in sums]],
        [VMEM((CHUNKS, XS, YS, ROWS, CHUNK), LOW), VMEM((CHUNKS, XS, YS, ROWS, CHUNK), LOW), VMEM((XS, YS, DOWN, WIDTH), LOW), VMEM((HEAD, HEADS * BQ), WIDE),
         VMEM((TOKENS, HEAD), WIDE), VMEM((TOKENS, HEAD), WIDE), VMEM((BK, STRIP), jnp.int32)]
        + Scatter.scratch(CHUNKS, ROWS, CHUNK) + Scatter.scratch(CHUNKS, ROWS, CHUNK) + Scatter.scratch(1, ROWS, WIDTH) + Scatter.scratch(1, DOWN, WIDTH - BY_Z)
        + ScatterZ.scratch(BY_Z) + pairs((4, 4), (4, 4), (7,), (4,)),
        2 * TOKENS * (WIDTH * 3 * FF + 3 * HEADS * TOKENS * HEAD), 1)


def tail_kernel(x, dh, dq, dk, dv, w, nc, ns, fc, fs, sum_o, sum_g, sum_u, sum_d, sum_z, dx, out_q, out_k, out_v, out_o, out_g, out_u, out_d,
                by_s, dw_s, terms, own, *rest):
    i = pl.program_id(0)
    steps = TOKENS // TB
    sems = paired(rest[26:])
    of = lambda n: rest[3 * n : 3 * n + 3]
    one = Scatter(0, True, lambda s, to: terms.at[0, to], own.at[:1], of(0), sems)
    two = Scatter(1, False, lambda s, to: terms.at[1, :, to], own.at[1:], of(1), sems)
    gate, up, out, down, last_one, last_two = [Last(n, ref, of(2 + n), sems[2]) for n, ref in enumerate((sum_g, sum_u, sum_o, sum_d, own.at[:1], own.at[1:]))]
    down_z = LastY(sum_z, rest[24:26], sems[3])

    def put(ref, first=0):
        def store(s, value):
            ref[0, :, first + s * value.shape[1] : first + (s + 1) * value.shape[1]] = value
        return store

    @on(0)
    def _():
        for item in (gate, up, out, down, last_one, last_two):
            item.clear()
        meet(False)
        for item in (down_z, out, gate, up, down):
            item.send()

    @pl.when(i < steps)
    def _():
        mine = tile(i, TB)
        for n in range(TB // SUB):
            cos, sin = angles(nc, ns, fc, fs, i * (TB // SUB) + n)
            r = slice(n * SUB, n * SUB + SUB)
            here = pl.ds(many(i, TB) + n * SUB, SUB)
            for h in range(HEADS + 1):
                t = (dq[h, r, :] if h < HEADS else dk[r, :]).astype(WIDE)
                by_s[here, h * HEAD : h * HEAD + HEAD] = (t * cos - pltpu.roll(t, HEAD // 2, 1) * sin).astype(LOW)
        by_s[mine, KEYS + HEAD :] = dv[:]
        term = t_mm(scaled(x[:])[2], by_s[mine, :])

        @on(0)
        def _():
            dw_s[:] = term

        @pl.when((i > 0) & (i < steps - 1))
        def _():
            dw_s[:] += term

        @on(steps - 1)
        def _():
            total = (dw_s[:] + term).astype(LOW)
            half = QKV // 2
            for n, item in enumerate((one, two)):
                terms[n] = total[:, n * half : n * half + half].reshape(XS, YS, ROWS, half)
                start(item.first(0))

    @on(steps + 2)
    def _():
        one.add_first()
        two.add_first()
        down_z.receive(functools.partial(put(out_d), 0))
        out.receive(put(out_o))
        gate.receive(put(out_g))
        up.receive(put(out_u))
        down.receive(put(out_d, BY_Z))

    @pl.when(i >= steps)
    def _():
        mine = tile(i - steps, TB)
        h, scale, _ = scaled(x[:])
        dx[:] = (dh[:].astype(WIDE) + unscaled(mm_t(by_s[mine, :], w[:]), h, scale)).astype(LOW)

    @on(2 * steps - 1)
    def _():
        one.add_second()
        last_one.send()
        two.add_second()
        last_two.send()

        def store_one(s, value):
            out_q[0, :, : QKV // 2] = value

        def store_two(s, value):
            out_q[0, :, QKV // 2 :] = value[:, : KEYS - QKV // 2]
            out_k[0] = value[:, KEYS - QKV // 2 : KEYS - QKV // 2 + HEAD]
            out_v[0] = value[:, KEYS - QKV // 2 + HEAD :]

        last_one.receive(store_one)
        last_two.receive(store_two)
        one.finish()
        two.finish()


def tail(x, dh, dq, dk, dv, w, sums):
    steps = TOKENS // TB
    early, late, both = (lambda i: jnp.minimum(i, steps - 1)), (lambda i: jnp.maximum(i - steps, 0)), (lambda i: i % steps)
    token = block(TB, HEAD, at=early)
    results = [(EACH, KEYS), (EACH, HEAD), (EACH, HEAD), (EACH, WIDTH), (EACH, FF), (EACH, FF), (TILE, WIDTH)]
    half = (1, ROWS, QKV // 2)
    forms = [(CHUNKS, ROWS, CHUNK), (CHUNKS, ROWS, CHUNK), (1, ROWS, WIDTH), (1, DOWN, WIDTH - BY_Z), half, half]
    return call(
        tail_kernel, "tail", 2 * steps,
        [(x, block(TB, WIDTH, at=both)), (dh, block(TB, WIDTH, at=late)), (dq, block(HEADS, TB, HEAD, at=early, dim=1)), (dk, token), (dv, token),
         (w, whole(WIDTH, QKV)), *tables(), *[(s, whole(*s.shape)) for s in sums]],
        [(low(TOKENS, WIDTH), block(TB, WIDTH, at=late)), *[(low(1, *s), whole(1, *s)) for s in results]],
        [VMEM((TOKENS, QKV), LOW), VMEM((WIDTH, QKV), WIDE), VMEM((2, XS, YS, ROWS, QKV // 2), LOW), VMEM((2, ROWS, QKV // 2), WIDE)]
        + [s for form in (half, half) for s in Scatter.scratch(*form)] + [s for form in forms for s in Last.scratch(*form)] + LastY.scratch(BY_Z)
        + pairs((2, 4), (2, 4), (6, 7), (4,)),
        4 * TOKENS * WIDTH * QKV, 2)


def solution(mesh):
    def step(x, dy, *weights):
        x, dy = x[0], dy[0]
        q, k, v, o, ot, lse, w, wo, gu, wd = front(x, weights)
        act, by_gate, by_up, bt, dh, by_o, delta, dwo = mlp(x, dy, o, ot, wo.reshape(KEYS, WIDTH), gu.reshape(WIDTH, 2 * FF), wd.reshape(FF, WIDTH))
        dq, dk, dv, *sums = back(bt, dy, act, by_gate, by_up, dwo.reshape(XS, YS, ROWS, WIDTH), q, k, v, by_o, lse, delta)
        dx, *by_weights = tail(x, dh, dq, dk, dv, w.reshape(WIDTH, QKV), sums)
        return dx[None], *by_weights

    states, cut = P(("rep", "dp"), None, None), P(None, "dp", None)
    return jax.shard_map(
        step,
        mesh=mesh,
        in_specs=(states, states) + (cut,) * 7,
        out_specs=(states,) + (P("rep", "dp", None),) * 7,
        check_vma=False,
    )
```

```python
import functools

import jax
import jax.numpy as jnp
import numpy as np
from jax import lax
from jax.experimental import pallas as pl
from jax.experimental.pallas import tpu as pltpu
from jax.sharding import PartitionSpec as P

NEG = -1e30
HIDDEN = 2 * NEG
LOG2E = 1.4426950408889634
TOKENS, WIDTH, HEADS, HEAD, FF, THETA = 2048, 768, 6, 128, 2048, 10000
QKV, KEYS = 1024, HEADS * HEAD
LOW, WIDE = jnp.bfloat16, jnp.float32
TB = 512
SUB = 128
SCALE = HEAD**-0.5
E = SCALE * LOG2E
BK, STRIP = 512, 512
BQ = 256
CHUNK = 256
XS, YS, ZS = 4, 4, 8
FOUR = (1, 2, 3)
EIGHT = tuple(range(1, ZS))
ROWS = WIDTH // (XS * YS)
EACH = ROWS // ZS
TILE = 16
DOWN = FF // (XS * YS)
ALL = slice(None)
VMEM, DMA = pltpu.VMEM, pltpu.SemaphoreType.DMA


def _dot(a, b, ca, cb):
    return lax.dot_general(a, b, (((ca,), (cb,)), ((), ())), preferred_element_type=WIDE)


def mm(a, b):
    return _dot(a, b, 1, 0)


def mm_t(a, b):
    return _dot(a, b, 1, 1)


def t_mm(a, b):
    return _dot(a, b, 0, 0)


def low(*shape):
    return jax.ShapeDtypeStruct(shape, LOW)


def wide(*shape):
    return jax.ShapeDtypeStruct(shape, WIDE)


def many(n, size):
    return pl.multiple_of(n * size, size)


def tile(n, size=TILE):
    return pl.ds(many(n, size), size)


def block(*shape, at=lambda i: i, dim=0):
    return pl.BlockSpec(shape, lambda i: tuple(at(i) if n == dim else 0 for n in range(len(shape))))


def whole(*shape):
    return pl.BlockSpec(shape, lambda i: (0,) * len(shape), pipeline_mode=pl.Buffered(1))


def call(kernel, name, steps, ins, outs, scratch, flops, number=None):
    more = {} if number is None else {"collective_id": number, "has_side_effects": True}
    moved = sum(a.size * a.dtype.itemsize for a, _ in (*ins, *outs))
    return pl.pallas_call(
        kernel,
        name=name,
        grid=(steps,),
        in_specs=[s for _, s in ins],
        out_specs=[s for _, s in outs],
        out_shape=[a for a, _ in outs],
        scratch_shapes=scratch,
        compiler_params=pltpu.CompilerParams(dimension_semantics=("arbitrary",), vmem_limit_bytes=67_000_000, **more),
        cost_estimate=pl.CostEstimate(flops=flops, bytes_accessed=moved, transcendentals=0),
    )(*[a for a, _ in ins])


def on(n):
    return pl.when(pl.program_id(0) == n)


def always(f):
    f()


MESH = pl.DeviceIdType.MESH
NEXT = (1, 3)


def place():
    me = lax.axis_index("dp")
    return lax.axis_index("rep"), me // (YS * ZS), (me // ZS) % YS, me % ZS


def at(x, y, z):
    return {"dp": (x * YS + y) * ZS + z}


def greet(sibling):
    c, x, y, z = place()
    devices = [at(x, y, (z + d) % ZS) for d in EIGHT] + [at(x, (y + d) % YS, z) for d in FOUR] + [at((x + d) % XS, y, z) for d in FOUR]
    devices += [{"rep": 1 - c}] if sibling else []
    barrier = pltpu.get_barrier_semaphore()
    for device in devices:
        pl.semaphore_signal(barrier, inc=1, device_id=device, device_id_type=MESH)


def met(sibling):
    pl.semaphore_wait(pltpu.get_barrier_semaphore(), len(EIGHT) + len(FOUR) + len(FOUR) + sibling)


def remote(src, dst, sems, at_sem, device):
    return pltpu.make_async_remote_copy(src_ref=src, dst_ref=dst, send_sem=sems[0].at[at_sem], recv_sem=sems[1].at[at_sem], device_id=device, device_id_type=MESH)


def start(copies):
    for copy in copies:
        copy.start()


def arrive(copies):
    for copy in copies:
        copy.wait_recv()


def leave(copies):
    for copy in copies:
        copy.wait_send()


class Gather:
    def __init__(self, number, out, buf, cut, sems):
        self.number, self.out, self.buf, self.sems = number, out, buf, sems
        self.c, self.x, self.y, self.z = place()
        self.half = out.shape[3] // 2
        self.a, self.b = (pl.ds(pl.multiple_of(self.c * self.half + s, HEAD), n) for s, n in ((0, cut), (cut, self.half - cut)))
        self.other = {"rep": 1 - self.c}

    def along_z(self):
        own = self.buf.at[self.z]
        return [remote(own, own, self.sems[0], (self.number, d - 1), at(self.x, self.y, (self.z + d) % ZS)) for d in EIGHT]

    def assemble(self, tmp):
        half = self.half
        for j in range(ZS):
            tmp[EACH * j : EACH * j + EACH, :half] = self.buf[j, :EACH, :].astype(WIDE)
        for n in range(2):
            @pl.when(self.c == n)
            def _():
                self.out[self.x, self.y, :, n * half : n * half + half] = tmp[:, :half].astype(LOW)

    def to_x(self, ref, sems, at_sem, ds=FOUR):
        return [remote(ref, ref, sems, (self.number, *at_sem, d), at((self.x + d) % XS, self.y, self.z)) for d in ds]

    def to_y(self, ref, sems, at_sem, ds=FOUR):
        return [remote(ref, ref, sems, (self.number, *at_sem, d), at(self.x, (self.y + d) % YS, self.z)) for d in ds]

    def second_a(self):
        return self.to_y(self.out.at[self.x, self.y, :, self.a], self.sems[1], (0,))

    def second_b(self):
        return self.to_x(self.out.at[self.x, self.y, :, self.b], self.sems[1], (1,))

    def third_a(self, ds=FOUR):
        return self.to_x(self.out.at[self.x, :, :, self.a], self.sems[2], (0,), ds)

    def third_b(self, ds=FOUR):
        return self.to_y(self.out.at[:, self.y, :, self.b], self.sems[2], (1,), ds)

    def relay_a(self):
        left, right = ((self.x + d) % XS for d in (3, 1))
        return [remote(ref, ref, self.sems[2], (self.number, 0, n), at(to, self.y, self.z)) for ref, n, to in (
            (self.out.at[left, :2, :, self.a], 0, right), (self.out.at[right, 2:, :, self.a], 2, left))]

    def relay_b(self):
        left, right = ((self.y + d) % YS for d in (3, 1))
        return [remote(ref, ref, self.sems[2], (self.number, 1, n), at(self.x, to, self.z)) for ref, n, to in (
            (self.out.at[:2, left, :, self.b], 0, right), (self.out.at[2:, right, :, self.b], 2, left))]

    def cross_a(self, d):
        got = self.out.at[(self.x - d + XS) % XS, :, :, self.a]
        return [remote(got, got, self.sems[3], (self.number, 0, d), self.other)]

    def cross_b(self, d):
        got = self.out.at[:, (self.y - d + YS) % YS, :, self.b]
        return [remote(got, got, self.sems[3], (self.number, 1, d), self.other)]

    def spread(self, ds=NEXT):
        arrive(self.second_a())
        start(self.third_a(ds))
        arrive(self.second_b())
        start(self.third_b(ds) + self.cross_a(0) + self.cross_b(0))

    def cross(self):
        for d in (1, 3, 2):
            arrive(self.third_a((d,)))
            start(self.cross_a(d))
            arrive(self.third_b((d,)))
            start(self.cross_b(d))

    def relay(self):
        arrive(self.third_a(NEXT))
        start(self.relay_a())
        arrive(self.third_b(NEXT))
        start(self.relay_b() + [copy for d in NEXT for copy in self.cross_a(d) + self.cross_b(d)])

    def relayed(self):
        arrive(self.relay_a())
        start(self.cross_a(2))
        arrive(self.relay_b())
        start(self.cross_b(2))

    def crossed(self):
        for d in range(XS):
            arrive(self.cross_a(d) + self.cross_b(d))

    def finish(self, ds=NEXT):
        leave(self.along_z() + self.second_a() + self.second_b() + self.third_a(ds) + self.third_b(ds))
        if ds == NEXT:
            leave(self.relay_a() + self.relay_b())
        for d in range(XS):
            leave(self.cross_a(d) + self.cross_b(d))


class GatherZ:
    def __init__(self, out, sems):
        self.out, self.sems = out, sems
        self.c, self.x, self.y, self.z = place()
        self.half = out.shape[3] // 2
        self.cols = pl.ds(pl.multiple_of(self.c * self.half, HEAD), self.half)

    def first(self):
        own = self.out.at[self.x, self.y, tile(self.z), self.cols]
        return [remote(own, own, self.sems[0], d, at((self.x + d) % XS, self.y, self.z)) for d in FOUR]

    def second(self):
        own = self.out.at[:, self.y, tile(self.z), self.cols]
        return [remote(own, own, self.sems[1], d, at(self.x, (self.y + d) % YS, self.z)) for d in FOUR]

    def third(self):
        own = self.out.at[:, :, tile(self.z), self.cols]
        return [remote(own, own, self.sems[2], d, at(self.x, self.y, (self.z + d) % ZS)) for d in EIGHT]

    def cross(self):
        own = self.out.at[:, :, :, self.cols]
        return [remote(own, own, self.sems[3], 0, {"rep": 1 - self.c})]

    def finish(self):
        leave(self.first() + self.second() + self.third() + self.cross())


class Scatter:
    @staticmethod
    def scratch(chunks, rows, cols):
        return [VMEM((3, chunks, 4, rows, cols), LOW), VMEM((4, chunks, rows, cols), LOW), VMEM((3, chunks, rows, cols), LOW)]

    def __init__(self, number, x_first, term, own, bufs, sems):
        self.number, self.term, self.own, self.sems = number, term, own, sems
        self.got, self.part, self.got2 = bufs
        c, x, y, self.z = place()
        self.p, self.q = (x, y) if x_first else (y, x)
        self.chip = (lambda p, q, z: at(p, q, z)) if x_first else (lambda p, q, z: at(q, p, z))
        self.chunks, self.rows, cols = own.shape
        self.step = {ROWS: ROWS, DOWN: DOWN // 2}[self.rows] if cols <= CHUNK else TILE

    def first(self, s):
        return [remote(self.term(s, (self.p + d) % 4), self.got.at[d - 1, s], self.sems[0], (self.number, d), self.chip((self.p + d) % 4, self.q, self.z)) for d in FOUR]

    def first_all(self):
        return [remote(self.got.at[d - 1], self.got.at[d - 1], self.sems[0], (self.number, d), self.chip((self.p + d) % 4, self.q, self.z)) for d in FOUR]

    def second(self):
        return [remote(self.part.at[(self.q + d) % 4], self.got2.at[d - 1], self.sems[1], (self.number, d), self.chip(self.p, (self.q + d) % 4, self.z)) for d in FOUR]

    def add_first(self):
        arrive(self.first_all())
        per = self.rows // self.step

        def total(s, b, r):
            total = self.term(s, self.p)[b, r, :].astype(WIDE)
            for d in FOUR:
                total += self.got[d - 1, s, b, r, :].astype(WIDE)
            return total

        def add(k, _):
            s, b, r = k // (3 * per), (self.q + 1 + k // per % 3) % 4, tile(k % per, self.step)
            self.part[b, s, r, :] = total(s, b, r).astype(LOW)

        lax.fori_loop(0, self.chunks * 3 * per, add, None, unroll=2)
        start(self.second())

        def keep(k, _):
            s, r = k // per, tile(k % per, self.step)
            self.own[s, r, :] = total(s, self.q, r)

        lax.fori_loop(0, self.chunks * per, keep, None)

    def add_second(self):
        arrive(self.second())
        per = self.rows // self.step

        def add(k, _):
            s, r = k // per, tile(k % per, self.step)
            total = self.own[s, r, :]
            for d in FOUR:
                total += self.got2[d - 1, s, r, :].astype(WIDE)
            self.own[s, r, :] = total

        lax.fori_loop(0, self.chunks * per, add, None)

    def finish(self):
        leave(self.first_all() + self.second())


class Last:
    @staticmethod
    def scratch(chunks, rows, cols):
        each = max(rows // ZS, 8)
        return [VMEM((ZS, chunks, each, cols), LOW), VMEM((ZS - 1, chunks, each, cols), LOW), VMEM((chunks, each, cols), WIDE)]

    def __init__(self, number, sums, bufs, sems):
        self.number, self.sums, self.sems = number, sums, sems
        self.packed, self.got, self.own = bufs
        self.chunks, rows, _ = sums.shape
        self.each = rows // ZS
        c, self.x, self.y, self.z = place()

    def clear(self):
        if self.each < 8:
            self.packed[:] = jnp.zeros_like(self.packed)

    def copies(self):
        return [remote(self.packed.at[(self.z + d) % ZS], self.got.at[d - 1], self.sems, (self.number, d - 1), at(self.x, self.y, (self.z + d) % ZS)) for d in EIGHT]

    def send(self):
        each = self.each

        def pack(s, _):
            for j in range(ZS):
                self.packed[j, s, :each, :] = self.sums[s, j * each : j * each + each, :].astype(LOW)

        lax.fori_loop(0, self.chunks, pack, None)
        start(self.copies())
        for j in range(ZS):
            @pl.when(self.z == j)
            def _():
                for s in range(self.chunks):
                    self.own[s, :each, :] = self.sums[s, j * each : j * each + each, :]

    def receive(self, store):
        arrive(self.copies())
        for s in range(self.chunks):
            total = self.own[s, : self.each, :]
            for d in EIGHT:
                total += self.got[d - 1, s, : self.each, :].astype(WIDE)
            store(s, total.astype(LOW))
        leave(self.copies())


class ScatterZ:
    @staticmethod
    def scratch(cols):
        return [VMEM((ZS - 1, XS, YS, TILE, cols), LOW), VMEM((XS, YS, TILE, cols), LOW), VMEM((3, YS, TILE, cols), LOW)]

    def __init__(self, terms, own, bufs, sems):
        self.terms, self.own, self.sems = terms, own, sems
        self.got, self.part, self.got2 = bufs
        c, self.x, self.y, self.z = place()
        self.cols = pl.ds(0, self.got.shape[4])

    def first(self, s):
        x, y = s // 2, pl.ds(s % 2 * 2, 2)
        return [remote(self.terms.at[x, y, tile((self.z + d) % ZS), self.cols], self.got.at[d - 1, x, y], self.sems[0], d - 1, at(self.x, self.y, (self.z + d) % ZS)) for d in EIGHT]

    def first_all(self):
        return [remote(self.got.at[d - 1], self.got.at[d - 1], self.sems[0], d - 1, at(self.x, self.y, (self.z + d) % ZS)) for d in EIGHT]

    def second(self):
        return [remote(self.part.at[(self.x + d) % XS], self.got2.at[d - 1], self.sems[1], d, at((self.x + d) % XS, self.y, self.z)) for d in FOUR]

    def add_first(self):
        arrive(self.first_all())

        def total(x, y):
            total = self.terms[x, y, tile(self.z), self.cols].astype(WIDE)
            for d in EIGHT:
                total += self.got[d - 1, x, y].astype(WIDE)
            return total

        def add(k, _):
            x, y = (self.x + 1 + k // YS) % XS, k % YS
            self.part[x, y] = total(x, y).astype(LOW)

        lax.fori_loop(0, len(FOUR) * YS, add, None, unroll=2)
        start(self.second())

        def keep(y, _):
            self.own[y] = total(self.x, y)

        lax.fori_loop(0, YS, keep, None)

    def add_second(self):
        arrive(self.second())

        def add(y, _):
            total = self.own[y]
            for d in FOUR:
                total += self.got2[d - 1, y].astype(WIDE)
            self.own[y] = total

        lax.fori_loop(0, YS, add, None)

    def finish(self):
        leave(self.first_all() + self.second())


class LastY:
    @staticmethod
    def scratch(cols):
        return [VMEM((YS, TILE, cols), LOW), VMEM((3, TILE, cols), LOW)]

    def __init__(self, sums, bufs, sems):
        self.sums, self.sems = sums, sems
        self.packed, self.got = bufs
        c, self.x, self.y, self.z = place()

    def copies(self):
        return [remote(self.packed.at[(self.y + d) % YS], self.got.at[d - 1], self.sems, d, at(self.x, (self.y + d) % YS, self.z)) for d in FOUR]

    def send(self):
        self.packed[:] = self.sums[:].astype(LOW)
        start(self.copies())

    def receive(self, store):
        arrive(self.copies())
        total = self.sums[self.y]
        for d in FOUR:
            total += self.got[d - 1].astype(WIDE)
        store(total.astype(LOW))
        leave(self.copies())


def pairs(*shapes):
    return [DMA(s) for s in shapes for _ in range(2)]


def paired(refs):
    return [refs[n : n + 2] for n in range(0, len(refs), 2)]


def tables():
    rate = float(THETA) ** (-np.arange(HEAD // 2, dtype=np.float64) / (HEAD // 2))
    rate = np.concatenate([rate, rate])
    near, far = (np.arange(0, n, s)[:, None] * rate for n, s in ((SUB, 1), (TOKENS, SUB)))
    arrays = [jnp.asarray(f(t).reshape(s), WIDE) for t, s in ((near, near.shape), (far, (TOKENS // SUB, 1, HEAD))) for f in (np.cos, np.sin)]
    return [(a, whole(*a.shape)) for a in arrays]


def angles(near_cos, near_sin, far_cos, far_sin, n):
    nc, ns, fc, fs = near_cos[:], near_sin[:], far_cos[n], far_sin[n]
    sign = jnp.where(lax.broadcasted_iota(jnp.int32, (1, HEAD), 1) < HEAD // 2, -1.0, 1.0)
    return fc * nc - fs * ns, (fs * nc + fc * ns) * sign


def scaled(h):
    h = h.astype(WIDE)
    scale = lax.rsqrt(jnp.mean(h * h, -1, keepdims=True) + 1e-6)
    return h, scale, (h * scale).astype(LOW)


def unscaled(by, h, scale):
    by = by.astype(LOW).astype(WIDE)
    return (by * scale - h * (scale * scale * scale * jnp.mean(by * h, -1, keepdims=True))).astype(LOW).astype(WIDE)


def front_kernel(x, wq, wk, wv, wo, wg, wu, wd, nc, ns, fc, fs, q, k, v, o, ot, lse, q_out, o_out, g_out, d_out,
                 q_w, o_w, g_w, d_w, q_z, o_z, g_z, tmp, k_s, v_s, top_s, mix_s, gap_s, done, *sems):
    i = pl.program_id(0)
    cols = HEADS * TB
    strips = range(0, cols, STRIP)
    sems = paired(sems)
    written = [pltpu.make_async_copy(src, dst, done.at[n]) for n, (src, dst) in enumerate(((q_w, q_out), (o_w, o_out), (g_w, g_out), (d_w, d_out)))]
    proj, out, gate = [Gather(n, *args, sems) for n, args in enumerate(((q_w, q_z, 256), (o_w, o_z, 256), (g_w, g_z, FF // 2)))]
    down = GatherZ(d_w, sems[4:])

    @on(0)
    def _():
        greet(True)
        c, x_, y_, z_ = place()
        rest = (gate, out)

        @pl.when(c == 0)
        def _():
            q_z[z_, :EACH, :] = wq[0, :, : QKV // 2]

        @pl.when(c == 1)
        def _():
            q_z[z_, :EACH, : KEYS - QKV // 2] = wq[0, :, QKV // 2 :]
            q_z[z_, :EACH, KEYS - QKV // 2 : KEYS - QKV // 2 + HEAD] = wk[0]
            q_z[z_, :EACH, KEYS - QKV // 2 + HEAD :] = wv[0]

        for buf in (q_z, o_z, g_z):
            buf[z_, EACH:, :] = jnp.zeros((buf.shape[1] - EACH, buf.shape[2]), LOW)
        met(True)
        start(proj.along_z())
        for n, w in enumerate((wg, wu)):
            @pl.when(c == n)
            def _():
                g_z[z_, :EACH, :] = w[0]
                o_z[z_, :EACH, :] = wo[0, :, n * out.half : n * out.half + out.half]
                d_w[x_, y_, tile(z_), n * down.half : n * down.half + down.half] = wd[0, :, n * down.half : n * down.half + down.half]
        start(down.first())
        for item in rest:
            start(item.along_z())
        gap_s[:] = lax.broadcasted_iota(jnp.int32, (BK, STRIP), 1) - lax.broadcasted_iota(jnp.int32, (BK, STRIP), 0)
        arrive(proj.along_z())
        proj.assemble(tmp)
        start(proj.second_a() + proj.second_b())
        arrive(down.first())
        start(down.second())
        proj.spread(FOUR)
        arrive(down.second())
        start(down.third())
        for item in rest:
            arrive(item.along_z())
            item.assemble(tmp)
            start(item.second_a() + item.second_b())
        proj.cross()
        proj.crossed()
        start(written[:1])

    a = scaled(x[:])[2]
    made = mm(a, q_w[:].reshape(WIDTH, QKV))
    mine = tile(i, TB)
    for n in range(TB // SUB):
        cos, sin = angles(nc, ns, fc, fs, i * (TB // SUB) + n)
        r = slice(n * SUB, n * SUB + SUB)
        for h in range(HEADS + 1):
            t = made[r, h * HEAD : h * HEAD + HEAD].astype(LOW).astype(WIDE)
            t = (t * cos + pltpu.roll(t, HEAD // 2, 1) * sin).astype(LOW)
            if h < HEADS:
                q[h, r, :] = t
            else:
                k[r, :] = t
    v[:] = made[:, KEYS + HEAD :].astype(LOW)
    k_s[mine, :] = k[:]
    v_s[mine, :] = v[:]

    @on(0)
    def _():
        gate.spread()

    top_s[:] = jnp.full((1, cols), NEG, WIDE)
    mix_s[:] = jnp.zeros((HEAD + 8, cols), WIDE)
    ones = jnp.ones((8, BK), LOW)

    def keys(j, masked):
        here = tile(j, BK)
        scores = [mm_t(k_s[here, :], q[:].reshape(cols, HEAD)[s : s + STRIP, :]) for s in strips]
        ok = gap_s[:] >= 0 if masked else None
        weights, keeps = [], []
        for s, score in zip(strips, scores):
            if masked:
                score = jnp.where(ok, score, HIDDEN)
            old = top_s[:, s : s + STRIP]
            top = jnp.maximum(old, score.max(axis=0, keepdims=True))
            top_s[:, s : s + STRIP] = top
            weights.append(jnp.exp2((score - top) * E).astype(LOW))
            keeps.append(jnp.exp2((old - top) * E))
        values = jnp.concatenate([v_s[here, :].T, ones], axis=0)
        for s, p, keep in zip(strips, weights, keeps):
            mix_s[:, s : s + STRIP] = mix_s[:, s : s + STRIP] * keep + mm(values, p)

    lax.fori_loop(0, i, lambda j, _: keys(j, False), None)

    @on(2)
    def _():
        out.relay()

    @on(3)
    def _():
        gate.crossed()
        start(written[2:3])
        out.relayed()
        arrive(down.third())
        start(down.cross())

    keys(i, True)
    total = mix_s[HEAD : HEAD + 1, :]
    result = mix_s[:HEAD, :] * (1 / total)
    lses = top_s[:] * SCALE + jnp.log(total)
    for h in range(HEADS):
        piece = result[:, h * TB : h * TB + TB].astype(LOW)
        ot[h] = piece
        o[h] = piece.T
        lse[h : h + 1, :] = lses[:, h * TB : h * TB + TB]

    @on(0)
    def _():
        out.spread()

    @on(1)
    def _():
        gate.relay()

    @on(2)
    def _():
        gate.relayed()

    @on(3)
    def _():
        out.crossed()
        arrive(down.cross())
        start(written[1::2])
        proj.finish(FOUR)
        for item in (gate, out, down):
            item.finish()
        for copy in written:
            copy.wait()


def front(x, weights):
    heads = (HEADS, TB, HEAD)
    matrices = [(XS, YS, ROWS, QKV), (XS, YS, ROWS, WIDTH), (XS, YS, ROWS, 2 * FF), (XS, YS, DOWN, WIDTH)]
    return call(
        front_kernel, "front", TOKENS // TB,
        [(x, block(TB, WIDTH)), *[(w, whole(*w.shape)) for w in weights], *tables()],
        [(low(HEADS, TOKENS, HEAD), block(*heads, dim=1)), (low(TOKENS, HEAD), block(TB, HEAD)), (low(TOKENS, HEAD), block(TB, HEAD)),
         (low(HEADS, TOKENS, HEAD), block(*heads, dim=1)), (low(HEADS, HEAD, TOKENS), block(HEADS, HEAD, TB, dim=2)), (wide(HEADS, TOKENS), block(HEADS, TB, dim=1)),
         *[(low(*s), pl.BlockSpec(memory_space=pl.ANY)) for s in matrices]],
        [VMEM(s, LOW) for s in matrices]
        + [VMEM((ZS, 8, n), LOW) for n in (QKV // 2, WIDTH // 2, FF)]
        + [VMEM((ROWS, FF), WIDE), VMEM((TOKENS, HEAD), LOW), VMEM((TOKENS, HEAD), LOW), VMEM((1, HEADS * TB), WIDE), VMEM((HEAD + 8, HEADS * TB), WIDE),
           VMEM((BK, STRIP), jnp.int32), DMA((4,))]
        + pairs((3, 7), (3, 2, 4), (3, 2, 4), (3, 2, 4), (4,), (4,), (8,), (1,)),
        2 * TOKENS * (WIDTH * QKV + HEADS * TOKENS * HEAD), 0)


def mlp_kernel(x_first, o_first, x_next, o_next, dy, o_last, dy_last, ot, wo, gu, wd, act, by_gu, bt, by_h, by_o, delta, dwo,
               h_s, scale_s, b_s, by_b_s, dh_s):
    i = pl.program_id(0)
    steps = TOKENS // TB
    every, dh_s = dh_s, dh_s.at[tile(jnp.maximum(i - 1, 0), TB)]

    def first(x, o, n):
        heads = jnp.concatenate([o[h] for h in range(HEADS)], axis=1)
        h = (x[:].astype(WIDE) + mm(heads, wo[:]).astype(LOW).astype(WIDE)).astype(LOW)
        _, scale, b = scaled(h)
        h_s[n % 3] = h
        scale_s[n % 3] = scale
        b_s[n % 2] = b

    def norm_back():
        n = (i + 2) % 3
        dh = (dy_last[:].astype(WIDE) + unscaled(by_b_s[:], h_s[n].astype(WIDE), scale_s[n])).astype(LOW)
        by_h[:] = dh
        dh_s[:] = dh

    def out_back():
        do = mm_t(dh_s[:], wo[:]).astype(LOW)
        for n in range(HEADS):
            piece = do[:, n * HEAD : n * HEAD + HEAD]
            by_o[n] = piece
            delta[n : n + 1, :] = (piece.astype(WIDE) * o_last[n].astype(WIDE)).T.sum(axis=0, keepdims=True)

    @on(0)
    def _():
        first(x_first, o_first, 0)

    @pl.when(i < steps)
    def _():
        b, dy_b = b_s[i % 2], dy[:]
        step = 1024

        def products(s):
            return mm(b, gu[:, s : s + step]), mm(b, gu[:, FF + s : FF + s + step]), mm_t(dy_b, wd[s : s + step, :]).astype(LOW)

        def between(s, g, u, by):
            f, f_up = slice(s, s + step), slice(FF + s, FF + s + step)
            by = by.astype(WIDE)
            sig = 0.5 * jnp.tanh(0.5 * g) + 0.5
            silu = g * sig
            act[:, f] = (silu * u).astype(LOW)
            by_gu[:, f_up] = (by * silu).astype(LOW)
            by_gu[:, f] = (by * u * (sig + silu * (1.0 - sig))).astype(LOW)

        made = products(0)
        norm_back()
        coming = products(step)
        between(0, *made)
        out_back()
        first(x_next, o_next, i + 1)
        between(step, *coming)
        bt[:] = b.T
        by_b_s[:] = mm_t(by_gu[:], gu[:])

    @on(steps)
    def _():
        norm_back()
        out_back()

        def rows(n, _):
            dwo[tile(n, SUB), :] = mm(ot[tile(n, SUB), :], every[:]).astype(LOW)

        lax.fori_loop(0, KEYS // SUB, rows, None)


def mlp(x, dy, o, ot, wo, gu, wd):
    steps = TOKENS // TB
    now, after, before = (lambda i: jnp.minimum(i, steps - 1)), (lambda i: jnp.minimum(i + 1, steps - 1)), (lambda i: jnp.maximum(i - 1, 0))
    rows = lambda at: block(TB, WIDTH, at=at)
    heads = lambda at: block(HEADS, TB, HEAD, at=at, dim=1)
    ff = lambda n: block(TB, n, at=now)
    return call(
        mlp_kernel, "mlp", steps + 1,
        [(x, whole(TB, WIDTH)), (o, whole(HEADS, TB, HEAD)), (x, rows(after)), (o, heads(after)), (dy, rows(now)), (o, heads(before)), (dy, rows(before)),
         *[(w, whole(*w.shape)) for w in (ot.reshape(KEYS, TOKENS), wo, gu, wd)]],
        [(low(TOKENS, FF), ff(FF)), (low(TOKENS, 2 * FF), ff(2 * FF)), (low(WIDTH, TOKENS), block(WIDTH, TB, at=now, dim=1)), (low(TOKENS, WIDTH), rows(before)),
         (low(HEADS, TOKENS, HEAD), heads(before)), (wide(HEADS, TOKENS), block(HEADS, TB, at=before, dim=1)), (low(KEYS, WIDTH), whole(KEYS, WIDTH))],
        [VMEM((3, TB, WIDTH), LOW), VMEM((3, TB, 1), WIDE), VMEM((2, TB, WIDTH), LOW), VMEM((TB, WIDTH), WIDE), VMEM((TOKENS, WIDTH), LOW)],
        2 * TOKENS * WIDTH * (3 * WIDTH + 5 * FF))


CHUNKS = FF // CHUNK
BY_Z = 512


def back_kernel(bt, dy, act, by_gate, by_up, dwo, q, k, v, do, lse, delta, dq, dk, dv, sum_o, sum_g, sum_u, sum_d, sum_z,
                dg_s, du_s, dd_s, dq_s, dk_s, dv_s, gap_s, *rest):
    i = pl.program_id(0)
    cols = HEADS * BQ
    strips = range(0, cols, STRIP)
    sems = paired(rest[15:])
    more = slice(BY_Z, WIDTH)
    of = lambda n: rest[3 * n : 3 * n + 3]
    gate = Scatter(0, True, lambda s, to: dg_s.at[s, to], sum_g, of(0), sems)
    up = Scatter(1, False, lambda s, to: du_s.at[s, :, to], sum_u, of(1), sems)
    out = Scatter(2, True, lambda s, to: dwo.at[to], sum_o, of(2), sems)
    down = Scatter(3, False, lambda s, to: dd_s.at[:, to, :, more], sum_d, of(3), sems)
    down_z = ScatterZ(dd_s, sum_z, of(4), sems[2:])

    @on(0)
    def _():
        place_ = lax.broadcasted_iota(jnp.int32, (BQ, STRIP), 1)
        gap_s[:] = jnp.where(place_ >= BQ, place_ - BQ, place_) - lax.broadcasted_iota(jnp.int32, (BQ, STRIP), 0)
        dk_s[:] = jnp.zeros_like(dk_s)
        dv_s[:] = jnp.zeros_like(dv_s)
        greet(False)

    @on(1)
    def _():
        met(False)
        start(out.first(0))

    @pl.when((i > 0) & (i <= CHUNKS))
    def _():
        start(down_z.first(i - 1) + gate.first(i - 1) + up.first(i - 1))

    @pl.when(i < CHUNKS)
    def _():
        dd_s[i // 2, pl.ds(i % 2 * 2, 2)] = t_mm(act[:], dy[:]).astype(LOW).reshape(2, DOWN, WIDTH)
        dg_s[i] = mm(bt[:], by_gate[:]).astype(LOW).reshape(XS, YS, ROWS, CHUNK)
        du_s[i] = mm(bt[:], by_up[:]).astype(LOW).reshape(XS, YS, ROWS, CHUNK)

    @on(CHUNKS)
    def _():
        start(down.first(0))

    @on(CHUNKS + 5)
    def _():
        for item in (out, gate, up, down, down_z):
            item.add_first()

    @pl.when(i >= CHUNKS)
    def _():
        iq = i - CHUNKS
        dq_s[:] = jnp.zeros_like(dq_s)
        lses = jnp.concatenate([lse[h : h + 1, :] for h in range(HEADS)], axis=1) * LOG2E
        deltas = jnp.concatenate([delta[h : h + 1, :] for h in range(HEADS)], axis=1)

        def keys(j, masked, size=BK):
            here = tile(j, size)
            qs = [q[:].reshape(cols, HEAD)[s : s + STRIP, :] for s in strips]
            dos = [do[:].reshape(cols, HEAD)[s : s + STRIP, :] for s in strips]
            scores = [mm_t(k[here, :], t) for t in qs]
            dps = [mm_t(v[here, :], t) for t in dos]
            kt = k[here, :].T
            ok = gap_s[:] >= 0 if masked else None
            for n, s in enumerate(strips):
                p = jnp.exp2(scores[n] * E - lses[:, s : s + STRIP])
                if masked:
                    p = jnp.where(ok, p, 0.0)
                ds = (p * (dps[n] - deltas[:, s : s + STRIP])).astype(LOW)
                dv_s[here, :] += mm(p.astype(LOW), dos[n])
                dk_s[here, :] += mm(ds, qs[n])
                dq_s[:, s : s + STRIP] += mm(kt, ds)

        full = iq * BQ // BK
        lax.fori_loop(0, full, lambda j, _: keys(j, False), None)

        @pl.when(iq % 2 == 1)
        def _():
            keys(iq - 1, False, BQ)

        keys(iq, True, BQ)
        for h in range(HEADS):
            dq[h] = (dq_s[:, h * BQ : h * BQ + BQ] * SCALE).T.astype(LOW)

    @on(CHUNKS + TOKENS // BQ - 1)
    def _():
        dk[:] = (dk_s[:] * SCALE).astype(LOW)
        dv[:] = dv_s[:].astype(LOW)

        for item in (down_z, out, gate, up, down):
            item.add_second()
            item.finish()


def back(bt, dy, act, by_gu, dwo, q, k, v, do, lse, delta):
    early, late = (lambda i: jnp.minimum(i, CHUNKS - 1)), (lambda i: jnp.maximum(i - CHUNKS, 0))
    cols = block(TOKENS, CHUNK, at=early, dim=1)
    heads, stats = block(HEADS, BQ, HEAD, at=late, dim=1), block(HEADS, BQ, at=late, dim=1)
    keys = whole(TOKENS, HEAD)
    sums = [(1, ROWS, WIDTH), (CHUNKS, ROWS, CHUNK), (CHUNKS, ROWS, CHUNK), (1, DOWN, WIDTH - BY_Z), (YS, TILE, BY_Z)]
    return call(
        back_kernel, "back", CHUNKS + TOKENS // BQ,
        [(bt, whole(WIDTH, TOKENS)), (dy, whole(TOKENS, WIDTH)), (act, cols), (by_gu, cols), (by_gu, block(TOKENS, CHUNK, at=lambda i: CHUNKS + early(i), dim=1)), (dwo, whole(*dwo.shape)),
         (q, heads), (k, keys), (v, keys), (do, heads), (lse, stats), (delta, stats)],
        [(low(HEADS, TOKENS, HEAD), heads), (low(TOKENS, HEAD), keys), (low(TOKENS, HEAD), keys), *[(wide(*s), whole(*s)) for s in sums]],
        [VMEM((CHUNKS, XS, YS, ROWS, CHUNK), LOW), VMEM((CHUNKS, XS, YS, ROWS, CHUNK), LOW), VMEM((XS, YS, DOWN, WIDTH), LOW), VMEM((HEAD, HEADS * BQ), WIDE),
         VMEM((TOKENS, HEAD), WIDE), VMEM((TOKENS, HEAD), WIDE), VMEM((BQ, STRIP), jnp.int32)]
        + Scatter.scratch(CHUNKS, ROWS, CHUNK) + Scatter.scratch(CHUNKS, ROWS, CHUNK) + Scatter.scratch(1, ROWS, WIDTH) + Scatter.scratch(1, DOWN, WIDTH - BY_Z)
        + ScatterZ.scratch(BY_Z) + pairs((4, 4), (4, 4), (7,), (4,)),
        2 * TOKENS * (WIDTH * 3 * FF + 3 * HEADS * TOKENS * HEAD), 1)


def tail_kernel(x, dh, dq, dk, dv, w, nc, ns, fc, fs, sum_o, sum_g, sum_u, sum_d, sum_z, dx, out_q, out_k, out_v, out_o, out_g, out_u, out_d,
                by_s, at_s, terms, own, *rest):
    i = pl.program_id(0)
    steps = TOKENS // TB
    sems = paired(rest[26:])
    of = lambda n: rest[3 * n : 3 * n + 3]
    one = Scatter(0, True, lambda s, to: terms.at[0, to], own.at[:1], of(0), sems)
    two = Scatter(1, False, lambda s, to: terms.at[1, :, to], own.at[1:], of(1), sems)
    gate, up, out, down, last_one, last_two = [Last(n, ref, of(2 + n), sems[2]) for n, ref in enumerate((sum_g, sum_u, sum_o, sum_d, own.at[:1], own.at[1:]))]
    down_z = LastY(sum_z, rest[24:26], sems[3])

    def put(ref, first=0):
        def store(s, value):
            ref[0, :, first + s * value.shape[1] : first + (s + 1) * value.shape[1]] = value
        return store

    @on(0)
    def _():
        greet(False)
        for item in (gate, up, out, down, last_one, last_two):
            item.clear()

    @pl.when(i < steps)
    def _():
        for n in range(TB // SUB):
            cos, sin = angles(nc, ns, fc, fs, i * (TB // SUB) + n)
            r = slice(n * SUB, n * SUB + SUB)
            here = pl.ds(many(i, TB) + n * SUB, SUB)
            for h in range(HEADS + 1):
                t = (dq[h, r, :] if h < HEADS else dk[r, :]).astype(WIDE)
                by_s[here, h * HEAD : h * HEAD + HEAD] = (t * cos - pltpu.roll(t, HEAD // 2, 1) * sin).astype(LOW)
        by_s[tile(i, TB), KEYS + HEAD :] = dv[:]
        at_s[i] = scaled(x[:])[2].T

    @pl.when((i >= steps) & (i < steps + 2))
    def _():
        half = tile(i - steps, QKV // 2)
        total = mm(at_s[0], by_s[:TB, half])
        for s in range(1, steps):
            total += mm(at_s[s], by_s[s * TB : s * TB + TB, half])
        terms[i - steps] = total.astype(LOW).reshape(XS, YS, ROWS, QKV // 2)

    @on(steps)
    def _():
        met(False)
        start(one.first(0))

    @on(steps + 1)
    def _():
        start(two.first(0))
        for item in (down_z, out, gate, up, down):
            item.send()

    @pl.when(i >= steps + 2)
    def _():
        mine = tile(i - steps - 2, TB)
        h, scale, _ = scaled(x[:])
        dx[:] = (dh[:].astype(WIDE) + unscaled(mm_t(by_s[mine, :], w[:]), h, scale)).astype(LOW)

    @on(2 * steps + 1)
    def _():
        one.add_first()
        two.add_first()
        down_z.receive(functools.partial(put(out_d), 0))
        out.receive(put(out_o))
        gate.receive(put(out_g))
        up.receive(put(out_u))
        down.receive(put(out_d, BY_Z))
        one.add_second()
        last_one.send()
        two.add_second()
        last_two.send()

        def store_one(s, value):
            out_q[0, :, : QKV // 2] = value

        def store_two(s, value):
            out_q[0, :, QKV // 2 :] = value[:, : KEYS - QKV // 2]
            out_k[0] = value[:, KEYS - QKV // 2 : KEYS - QKV // 2 + HEAD]
            out_v[0] = value[:, KEYS - QKV // 2 + HEAD :]

        last_one.receive(store_one)
        last_two.receive(store_two)
        one.finish()
        two.finish()


def tail(x, dh, dq, dk, dv, w, sums):
    steps = TOKENS // TB
    early, late = (lambda i: jnp.minimum(i, steps - 1)), (lambda i: jnp.maximum(i - steps - 2, 0))
    both = lambda i: jnp.where(i < steps, i, late(i))
    token = block(TB, HEAD, at=early)
    results = [(EACH, KEYS), (EACH, HEAD), (EACH, HEAD), (EACH, WIDTH), (EACH, FF), (EACH, FF), (TILE, WIDTH)]
    half = (1, ROWS, QKV // 2)
    forms = [(CHUNKS, ROWS, CHUNK), (CHUNKS, ROWS, CHUNK), (1, ROWS, WIDTH), (1, DOWN, WIDTH - BY_Z), half, half]
    return call(
        tail_kernel, "tail", 2 * steps + 2,
        [(x, block(TB, WIDTH, at=both)), (dh, block(TB, WIDTH, at=late)), (dq, block(HEADS, TB, HEAD, at=early, dim=1)), (dk, token), (dv, token),
         (w, whole(WIDTH, QKV)), *tables(), *[(s, whole(*s.shape)) for s in sums]],
        [(low(TOKENS, WIDTH), block(TB, WIDTH, at=late)), *[(low(1, *s), whole(1, *s)) for s in results]],
        [VMEM((TOKENS, QKV), LOW), VMEM((steps, WIDTH, TB), LOW), VMEM((2, XS, YS, ROWS, QKV // 2), LOW), VMEM((2, ROWS, QKV // 2), WIDE)]
        + [s for form in (half, half) for s in Scatter.scratch(*form)] + [s for form in forms for s in Last.scratch(*form)] + LastY.scratch(BY_Z)
        + pairs((2, 4), (2, 4), (6, 7), (4,)),
        4 * TOKENS * WIDTH * QKV, 2)


def publish_kernel(*refs):
    half = len(refs) // 2
    for src, dst in zip(refs[:half], refs[half:]):
        dst[:] = src[:]


def publish(dx, *rest):
    arrays = [(dx, block(TB, WIDTH)), *[(a, whole(*a.shape)) for a in rest]]
    return call(publish_kernel, "publish", TOKENS // TB, arrays, [(low(*a.shape), s) for a, s in arrays], [], 0)


def solution(mesh):
    def step(x, dy, *weights):
        x, dy = x[0], dy[0]
        q, k, v, o, ot, lse, w, wo, gu, wd = front(x, weights)
        act, by_gu, bt, dh, by_o, delta, dwo = mlp(x, dy, o, ot, wo.reshape(KEYS, WIDTH), gu.reshape(WIDTH, 2 * FF), wd.reshape(FF, WIDTH))
        dq, dk, dv, *sums = back(bt, dy, act, by_gu, dwo.reshape(XS, YS, ROWS, WIDTH), q, k, v, by_o, lse, delta)
        dx, *by_weights = publish(*tail(x, dh, dq, dk, dv, w.reshape(WIDTH, QKV), sums))
        return dx[None], *by_weights

    states, cut = P(("rep", "dp"), None, None), P(None, "dp", None)
    return jax.shard_map(
        step,
        mesh=mesh,
        in_specs=(states, states) + (cut,) * 7,
        out_specs=(states,) + (P("rep", "dp", None),) * 7,
        check_vma=False,
    )
```

```python
import functools

import jax
import jax.numpy as jnp
import numpy as np
from jax import lax
from jax.experimental import pallas as pl
from jax.experimental.pallas import tpu as pltpu
from jax.sharding import PartitionSpec as P

NEG = -1e30
HIDDEN = 2 * NEG
LOG2E = 1.4426950408889634
TOKENS, WIDTH, HEADS, HEAD, FF, THETA = 2048, 768, 6, 128, 2048, 10000
QKV, KEYS = 1024, HEADS * HEAD
LOW, WIDE = jnp.bfloat16, jnp.float32
TB = 512
SUB = 128
SCALE = HEAD**-0.5
E = SCALE * LOG2E
BK, STRIP = 512, 512
BQ = 256
CHUNK = 256
XS, YS, ZS = 4, 4, 8
FOUR = (1, 2, 3)
EIGHT = tuple(range(1, ZS))
ROWS = WIDTH // (XS * YS)
EACH = ROWS // ZS
TILE = 16
DOWN = FF // (XS * YS)
ALL = slice(None)
VMEM, DMA = pltpu.VMEM, pltpu.SemaphoreType.DMA


def _dot(a, b, ca, cb):
    return lax.dot_general(a, b, (((ca,), (cb,)), ((), ())), preferred_element_type=WIDE)


def mm(a, b):
    return _dot(a, b, 1, 0)


def mm_t(a, b):
    return _dot(a, b, 1, 1)


def t_mm(a, b):
    return _dot(a, b, 0, 0)


def low(*shape):
    return jax.ShapeDtypeStruct(shape, LOW)


def wide(*shape):
    return jax.ShapeDtypeStruct(shape, WIDE)


def many(n, size):
    return pl.multiple_of(n * size, size)


def tile(n, size=TILE):
    return pl.ds(many(n, size), size)


def block(*shape, at=lambda i: i, dim=0):
    return pl.BlockSpec(shape, lambda i: tuple(at(i) if n == dim else 0 for n in range(len(shape))))


def whole(*shape):
    return pl.BlockSpec(shape, lambda i: (0,) * len(shape), pipeline_mode=pl.Buffered(1))


def call(kernel, name, steps, ins, outs, scratch, flops, number=None):
    more = {} if number is None else {"collective_id": number, "has_side_effects": True}
    moved = sum(a.size * a.dtype.itemsize for a, _ in (*ins, *outs))
    return pl.pallas_call(
        kernel,
        name=name,
        grid=(steps,),
        in_specs=[s for _, s in ins],
        out_specs=[s for _, s in outs],
        out_shape=[a for a, _ in outs],
        scratch_shapes=scratch,
        compiler_params=pltpu.CompilerParams(dimension_semantics=("arbitrary",), vmem_limit_bytes=67_000_000, **more),
        cost_estimate=pl.CostEstimate(flops=flops, bytes_accessed=moved, transcendentals=0),
    )(*[a for a, _ in ins])


def on(n):
    return pl.when(pl.program_id(0) == n)


def always(f):
    f()


MESH = pl.DeviceIdType.MESH
NEXT = (1, 3)


def place():
    me = lax.axis_index("dp")
    return lax.axis_index("rep"), me // (YS * ZS), (me // ZS) % YS, me % ZS


def at(x, y, z):
    return {"dp": (x * YS + y) * ZS + z}


def greet(sibling):
    c, x, y, z = place()
    devices = [at(x, y, (z + d) % ZS) for d in EIGHT] + [at(x, (y + d) % YS, z) for d in FOUR] + [at((x + d) % XS, y, z) for d in FOUR]
    devices += [{"rep": 1 - c}] if sibling else []
    barrier = pltpu.get_barrier_semaphore()
    for device in devices:
        pl.semaphore_signal(barrier, inc=1, device_id=device, device_id_type=MESH)


def met(sibling):
    pl.semaphore_wait(pltpu.get_barrier_semaphore(), len(EIGHT) + len(FOUR) + len(FOUR) + sibling)


def remote(src, dst, sems, at_sem, device):
    return pltpu.make_async_remote_copy(src_ref=src, dst_ref=dst, send_sem=sems[0].at[at_sem], recv_sem=sems[1].at[at_sem], device_id=device, device_id_type=MESH)


def start(copies):
    for copy in copies:
        copy.start()


def arrive(copies):
    for copy in copies:
        copy.wait_recv()


def leave(copies):
    for copy in copies:
        copy.wait_send()


class Gather:
    def __init__(self, number, out, buf, cut, sems):
        self.number, self.out, self.buf, self.sems = number, out, buf, sems
        self.c, self.x, self.y, self.z = place()
        self.half = out.shape[3] // 2
        self.a, self.b = (pl.ds(pl.multiple_of(self.c * self.half + s, HEAD), n) for s, n in ((0, cut), (cut, self.half - cut)))
        self.other = {"rep": 1 - self.c}

    def along_z(self):
        own = self.buf.at[self.z]
        return [remote(own, own, self.sems[0], (self.number, d - 1), at(self.x, self.y, (self.z + d) % ZS)) for d in EIGHT]

    def assemble(self, tmp):
        half = self.half
        for j in range(ZS):
            tmp[EACH * j : EACH * j + EACH, :half] = self.buf[j, :EACH, :].astype(WIDE)
        for n in range(2):
            @pl.when(self.c == n)
            def _():
                self.out[self.x, self.y, :, n * half : n * half + half] = tmp[:, :half].astype(LOW)

    def to_x(self, ref, sems, at_sem, ds=FOUR):
        return [remote(ref, ref, sems, (self.number, *at_sem, d), at((self.x + d) % XS, self.y, self.z)) for d in ds]

    def to_y(self, ref, sems, at_sem, ds=FOUR):
        return [remote(ref, ref, sems, (self.number, *at_sem, d), at(self.x, (self.y + d) % YS, self.z)) for d in ds]

    def second_a(self):
        return self.to_y(self.out.at[self.x, self.y, :, self.a], self.sems[1], (0,))

    def second_b(self):
        return self.to_x(self.out.at[self.x, self.y, :, self.b], self.sems[1], (1,))

    def third_a(self, ds=FOUR):
        return self.to_x(self.out.at[self.x, :, :, self.a], self.sems[2], (0,), ds)

    def third_b(self, ds=FOUR):
        return self.to_y(self.out.at[:, self.y, :, self.b], self.sems[2], (1,), ds)

    def relay_a(self):
        left, right = ((self.x + d) % XS for d in (3, 1))
        return [remote(ref, ref, self.sems[2], (self.number, 0, n), at(to, self.y, self.z)) for ref, n, to in (
            (self.out.at[left, :2, :, self.a], 0, right), (self.out.at[right, 2:, :, self.a], 2, left))]

    def relay_b(self):
        left, right = ((self.y + d) % YS for d in (3, 1))
        return [remote(ref, ref, self.sems[2], (self.number, 1, n), at(self.x, to, self.z)) for ref, n, to in (
            (self.out.at[:2, left, :, self.b], 0, right), (self.out.at[2:, right, :, self.b], 2, left))]

    def cross_a(self, d):
        got = self.out.at[(self.x - d + XS) % XS, :, :, self.a]
        return [remote(got, got, self.sems[3], (self.number, 0, d), self.other)]

    def cross_b(self, d):
        got = self.out.at[:, (self.y - d + YS) % YS, :, self.b]
        return [remote(got, got, self.sems[3], (self.number, 1, d), self.other)]

    def spread(self, ds=NEXT):
        arrive(self.second_a())
        start(self.third_a(ds))
        arrive(self.second_b())
        start(self.third_b(ds) + self.cross_a(0) + self.cross_b(0))

    def cross(self):
        for d in (1, 3, 2):
            arrive(self.third_a((d,)))
            start(self.cross_a(d))
            arrive(self.third_b((d,)))
            start(self.cross_b(d))

    def relay(self):
        arrive(self.third_a(NEXT))
        start(self.relay_a())
        arrive(self.third_b(NEXT))
        start(self.relay_b() + [copy for d in NEXT for copy in self.cross_a(d) + self.cross_b(d)])

    def relayed(self):
        arrive(self.relay_a())
        start(self.cross_a(2))
        arrive(self.relay_b())
        start(self.cross_b(2))

    def crossed(self):
        for d in range(XS):
            arrive(self.cross_a(d) + self.cross_b(d))

    def finish(self, ds=NEXT):
        leave(self.along_z() + self.second_a() + self.second_b() + self.third_a(ds) + self.third_b(ds))
        if ds == NEXT:
            leave(self.relay_a() + self.relay_b())
        for d in range(XS):
            leave(self.cross_a(d) + self.cross_b(d))


class GatherZ:
    def __init__(self, out, sems):
        self.out, self.sems = out, sems
        self.c, self.x, self.y, self.z = place()
        self.half = out.shape[3] // 2
        self.cols = pl.ds(pl.multiple_of(self.c * self.half, HEAD), self.half)

    def first(self):
        own = self.out.at[self.x, self.y, tile(self.z), self.cols]
        return [remote(own, own, self.sems[0], d, at((self.x + d) % XS, self.y, self.z)) for d in FOUR]

    def second(self):
        own = self.out.at[:, self.y, tile(self.z), self.cols]
        return [remote(own, own, self.sems[1], d, at(self.x, (self.y + d) % YS, self.z)) for d in FOUR]

    def third(self):
        own = self.out.at[:, :, tile(self.z), self.cols]
        return [remote(own, own, self.sems[2], d, at(self.x, self.y, (self.z + d) % ZS)) for d in EIGHT]

    def cross(self):
        own = self.out.at[:, :, :, self.cols]
        return [remote(own, own, self.sems[3], 0, {"rep": 1 - self.c})]

    def finish(self):
        leave(self.first() + self.second() + self.third() + self.cross())


class Scatter:
    @staticmethod
    def scratch(chunks, rows, cols):
        return [VMEM((3, chunks, 4, rows, cols), LOW), VMEM((4, chunks, rows, cols), LOW), VMEM((3, chunks, rows, cols), LOW)]

    def __init__(self, number, x_first, term, own, bufs, sems):
        self.number, self.term, self.own, self.sems = number, term, own, sems
        self.got, self.part, self.got2 = bufs
        c, x, y, self.z = place()
        self.p, self.q = (x, y) if x_first else (y, x)
        self.chip = (lambda p, q, z: at(p, q, z)) if x_first else (lambda p, q, z: at(q, p, z))
        self.chunks, self.rows, cols = own.shape
        self.step = {ROWS: ROWS, DOWN: DOWN // 2}[self.rows] if cols <= CHUNK else TILE

    def first(self, s):
        return [remote(self.term(s, (self.p + d) % 4), self.got.at[d - 1, s], self.sems[0], (self.number, d), self.chip((self.p + d) % 4, self.q, self.z)) for d in FOUR]

    def first_all(self):
        return [remote(self.got.at[d - 1], self.got.at[d - 1], self.sems[0], (self.number, d), self.chip((self.p + d) % 4, self.q, self.z)) for d in FOUR]

    def second(self):
        return [remote(self.part.at[(self.q + d) % 4], self.got2.at[d - 1], self.sems[1], (self.number, d), self.chip(self.p, (self.q + d) % 4, self.z)) for d in FOUR]

    def add_first(self):
        arrive(self.first_all())
        per = self.rows // self.step

        def total(s, b, r):
            total = self.term(s, self.p)[b, r, :].astype(WIDE)
            for d in FOUR:
                total += self.got[d - 1, s, b, r, :].astype(WIDE)
            return total

        def add(k, _):
            s, b, r = k // (3 * per), (self.q + 1 + k // per % 3) % 4, tile(k % per, self.step)
            self.part[b, s, r, :] = total(s, b, r).astype(LOW)

        lax.fori_loop(0, self.chunks * 3 * per, add, None, unroll=2)
        start(self.second())

        def keep(k, _):
            s, r = k // per, tile(k % per, self.step)
            self.own[s, r, :] = total(s, self.q, r)

        lax.fori_loop(0, self.chunks * per, keep, None)

    def add_second(self):
        arrive(self.second())
        per = self.rows // self.step

        def add(k, _):
            s, r = k // per, tile(k % per, self.step)
            total = self.own[s, r, :]
            for d in FOUR:
                total += self.got2[d - 1, s, r, :].astype(WIDE)
            self.own[s, r, :] = total

        lax.fori_loop(0, self.chunks * per, add, None)

    def finish(self):
        leave(self.first_all() + self.second())


class Last:
    @staticmethod
    def scratch(chunks, rows, cols):
        each = max(rows // ZS, 8)
        return [VMEM((ZS, chunks, each, cols), LOW), VMEM((ZS - 1, chunks, each, cols), LOW), VMEM((chunks, each, cols), WIDE)]

    def __init__(self, number, sums, bufs, sems):
        self.number, self.sums, self.sems = number, sums, sems
        self.packed, self.got, self.own = bufs
        self.chunks, rows, _ = sums.shape
        self.each = rows // ZS
        c, self.x, self.y, self.z = place()

    def clear(self):
        if self.each < 8:
            self.packed[:] = jnp.zeros_like(self.packed)

    def copies(self):
        return [remote(self.packed.at[(self.z + d) % ZS], self.got.at[d - 1], self.sems, (self.number, d - 1), at(self.x, self.y, (self.z + d) % ZS)) for d in EIGHT]

    def send(self):
        each = self.each

        def pack(s, _):
            for j in range(ZS):
                self.packed[j, s, :each, :] = self.sums[s, j * each : j * each + each, :].astype(LOW)

        lax.fori_loop(0, self.chunks, pack, None)
        start(self.copies())
        for j in range(ZS):
            @pl.when(self.z == j)
            def _():
                for s in range(self.chunks):
                    self.own[s, :each, :] = self.sums[s, j * each : j * each + each, :]

    def receive(self, store):
        arrive(self.copies())
        for s in range(self.chunks):
            total = self.own[s, : self.each, :]
            for d in EIGHT:
                total += self.got[d - 1, s, : self.each, :].astype(WIDE)
            store(s, total.astype(LOW))
        leave(self.copies())


class ScatterZ:
    @staticmethod
    def scratch(cols):
        return [VMEM((ZS - 1, XS, YS, TILE, cols), LOW), VMEM((XS, YS, TILE, cols), LOW), VMEM((3, YS, TILE, cols), LOW)]

    def __init__(self, terms, own, bufs, sems):
        self.terms, self.own, self.sems = terms, own, sems
        self.got, self.part, self.got2 = bufs
        c, self.x, self.y, self.z = place()
        self.cols = pl.ds(0, self.got.shape[4])

    def first(self, s):
        x, y = s // 2, pl.ds(s % 2 * 2, 2)
        return [remote(self.terms.at[x, y, tile((self.z + d) % ZS), self.cols], self.got.at[d - 1, x, y], self.sems[0], d - 1, at(self.x, self.y, (self.z + d) % ZS)) for d in EIGHT]

    def first_all(self):
        return [remote(self.got.at[d - 1], self.got.at[d - 1], self.sems[0], d - 1, at(self.x, self.y, (self.z + d) % ZS)) for d in EIGHT]

    def second(self):
        return [remote(self.part.at[(self.x + d) % XS], self.got2.at[d - 1], self.sems[1], d, at((self.x + d) % XS, self.y, self.z)) for d in FOUR]

    def add_first(self):
        arrive(self.first_all())

        def total(x, y):
            total = self.terms[x, y, tile(self.z), self.cols].astype(WIDE)
            for d in EIGHT:
                total += self.got[d - 1, x, y].astype(WIDE)
            return total

        def add(k, _):
            x, y = (self.x + 1 + k // YS) % XS, k % YS
            self.part[x, y] = total(x, y).astype(LOW)

        lax.fori_loop(0, len(FOUR) * YS, add, None, unroll=2)
        start(self.second())

        def keep(y, _):
            self.own[y] = total(self.x, y)

        lax.fori_loop(0, YS, keep, None)

    def add_second(self):
        arrive(self.second())

        def add(y, _):
            total = self.own[y]
            for d in FOUR:
                total += self.got2[d - 1, y].astype(WIDE)
            self.own[y] = total

        lax.fori_loop(0, YS, add, None)

    def finish(self):
        leave(self.first_all() + self.second())


class LastY:
    @staticmethod
    def scratch(cols):
        return [VMEM((YS, TILE, cols), LOW), VMEM((3, TILE, cols), LOW)]

    def __init__(self, sums, bufs, sems):
        self.sums, self.sems = sums, sems
        self.packed, self.got = bufs
        c, self.x, self.y, self.z = place()

    def copies(self):
        return [remote(self.packed.at[(self.y + d) % YS], self.got.at[d - 1], self.sems, d, at(self.x, (self.y + d) % YS, self.z)) for d in FOUR]

    def send(self):
        self.packed[:] = self.sums[:].astype(LOW)
        start(self.copies())

    def receive(self, store):
        arrive(self.copies())
        total = self.sums[self.y]
        for d in FOUR:
            total += self.got[d - 1].astype(WIDE)
        store(total.astype(LOW))
        leave(self.copies())


def pairs(*shapes):
    return [DMA(s) for s in shapes for _ in range(2)]


def paired(refs):
    return [refs[n : n + 2] for n in range(0, len(refs), 2)]


def tables():
    rate = float(THETA) ** (-np.arange(HEAD // 2, dtype=np.float64) / (HEAD // 2))
    rate = np.concatenate([rate, rate])
    near, far = (np.arange(0, n, s)[:, None] * rate for n, s in ((SUB, 1), (TOKENS, SUB)))
    arrays = [jnp.asarray(f(t).reshape(s), WIDE) for t, s in ((near, near.shape), (far, (TOKENS // SUB, 1, HEAD))) for f in (np.cos, np.sin)]
    return [(a, whole(*a.shape)) for a in arrays]


def angles(near_cos, near_sin, far_cos, far_sin, n):
    nc, ns, fc, fs = near_cos[:], near_sin[:], far_cos[n], far_sin[n]
    sign = jnp.where(lax.broadcasted_iota(jnp.int32, (1, HEAD), 1) < HEAD // 2, -1.0, 1.0)
    return fc * nc - fs * ns, (fs * nc + fc * ns) * sign


def scaled(h):
    h = h.astype(WIDE)
    scale = lax.rsqrt(jnp.mean(h * h, -1, keepdims=True) + 1e-6)
    return h, scale, (h * scale).astype(LOW)


def unscaled(by, h, scale):
    by = by.astype(LOW).astype(WIDE)
    return (by * scale - h * (scale * scale * scale * jnp.mean(by * h, -1, keepdims=True))).astype(LOW).astype(WIDE)


def front_kernel(x_in, wq, wk, wv, wo, wg, wu, wd, nc, ns, fc, fs, q, k, v, o, ot, lse, at_out, q_out, o_out, g_out, d_out,
                 q_w, o_w, g_w, d_w, a_s, at_s, x, q_z, o_z, g_z, tmp, k_s, v_s, top_s, mix_s, gap_s, done, *sems):
    i = pl.program_id(0)
    cols = HEADS * TB
    strips = range(0, cols, STRIP)
    sems = paired(sems)
    written = [pltpu.make_async_copy(src, dst, done.at[n]) for n, (src, dst) in enumerate(((q_w, q_out), (o_w, o_out), (g_w, g_out), (d_w, d_out), (at_s, at_out)))]
    load = pltpu.make_async_copy(x_in, x, done.at[len(written)])
    proj, out, gate = [Gather(n, *args, sems) for n, args in enumerate(((q_w, q_z, 256), (o_w, o_z, 256), (g_w, g_z, FF // 2)))]
    down = GatherZ(d_w, sems[4:])

    @on(0)
    def _():
        greet(True)
        load.start()
        c, x_, y_, z_ = place()
        rest = (gate, out)

        @pl.when(c == 0)
        def _():
            q_z[z_, :EACH, :] = wq[0, :, : QKV // 2]

        @pl.when(c == 1)
        def _():
            q_z[z_, :EACH, : KEYS - QKV // 2] = wq[0, :, QKV // 2 :]
            q_z[z_, :EACH, KEYS - QKV // 2 : KEYS - QKV // 2 + HEAD] = wk[0]
            q_z[z_, :EACH, KEYS - QKV // 2 + HEAD :] = wv[0]

        for buf in (q_z, o_z, g_z):
            buf[z_, EACH:, :] = jnp.zeros((buf.shape[1] - EACH, buf.shape[2]), LOW)
        met(True)
        start(proj.along_z())
        for n, w in enumerate((wg, wu)):
            @pl.when(c == n)
            def _():
                g_z[z_, :EACH, :] = w[0]
                o_z[z_, :EACH, :] = wo[0, :, n * out.half : n * out.half + out.half]
                d_w[x_, y_, tile(z_), n * down.half : n * down.half + down.half] = wd[0, :, n * down.half : n * down.half + down.half]
        start(down.first())
        for item in rest:
            start(item.along_z())
        gap_s[:] = lax.broadcasted_iota(jnp.int32, (BK, STRIP), 1) - lax.broadcasted_iota(jnp.int32, (BK, STRIP), 0)

        def norm(n, _):
            a = scaled(x[tile(n, TB), :])[2]
            a_s[tile(n, TB), :] = a
            at_s[:, tile(n, TB)] = a.T

        load.wait()
        lax.fori_loop(0, TOKENS // TB, norm, None)
        start(written[4:])
        arrive(proj.along_z())
        proj.assemble(tmp)
        start(proj.second_a() + proj.second_b())
        arrive(down.first())
        start(down.second())
        proj.spread(FOUR)
        arrive(down.second())
        start(down.third())
        for item in rest:
            arrive(item.along_z())
            item.assemble(tmp)
            start(item.second_a() + item.second_b())
        proj.cross()
        proj.crossed()
        start(written[:1])

    mine = tile(i, TB)
    made = mm(a_s[mine, :], q_w[:].reshape(WIDTH, QKV))
    for n in range(TB // SUB):
        cos, sin = angles(nc, ns, fc, fs, i * (TB // SUB) + n)
        r = slice(n * SUB, n * SUB + SUB)
        for h in range(HEADS + 1):
            t = made[r, h * HEAD : h * HEAD + HEAD].astype(LOW).astype(WIDE)
            t = (t * cos + pltpu.roll(t, HEAD // 2, 1) * sin).astype(LOW)
            if h < HEADS:
                q[h, r, :] = t
            else:
                k[r, :] = t
    v[:] = made[:, KEYS + HEAD :].astype(LOW)
    k_s[mine, :] = k[:]
    v_s[mine, :] = v[:]

    @on(0)
    def _():
        gate.spread()

    top_s[:] = jnp.full((1, cols), NEG, WIDE)
    mix_s[:] = jnp.zeros((HEAD + 8, cols), WIDE)
    ones = jnp.ones((8, BK), LOW)

    def keys(j, masked):
        here = tile(j, BK)
        scores = [mm_t(k_s[here, :], q[:].reshape(cols, HEAD)[s : s + STRIP, :]) for s in strips]
        ok = gap_s[:] >= 0 if masked else None
        weights, keeps = [], []
        for s, score in zip(strips, scores):
            if masked:
                score = jnp.where(ok, score, HIDDEN)
            old = top_s[:, s : s + STRIP]
            top = jnp.maximum(old, score.max(axis=0, keepdims=True))
            top_s[:, s : s + STRIP] = top
            weights.append(jnp.exp2((score - top) * E).astype(LOW))
            keeps.append(jnp.exp2((old - top) * E))
        values = jnp.concatenate([v_s[here, :].T, ones], axis=0)
        for s, p, keep in zip(strips, weights, keeps):
            mix_s[:, s : s + STRIP] = mix_s[:, s : s + STRIP] * keep + mm(values, p)

    lax.fori_loop(0, i, lambda j, _: keys(j, False), None)

    @on(2)
    def _():
        out.relay()

    @on(3)
    def _():
        gate.crossed()
        start(written[2:3])
        out.relayed()
        arrive(down.third())
        start(down.cross())

    keys(i, True)
    total = mix_s[HEAD : HEAD + 1, :]
    result = mix_s[:HEAD, :] * (1 / total)
    lses = top_s[:] * SCALE + jnp.log(total)
    for h in range(HEADS):
        piece = result[:, h * TB : h * TB + TB].astype(LOW)
        ot[h] = piece
        o[h] = piece.T
        lse[h : h + 1, :] = lses[:, h * TB : h * TB + TB]

    @on(0)
    def _():
        out.spread()

    @on(1)
    def _():
        gate.relay()

    @on(2)
    def _():
        gate.relayed()

    @on(3)
    def _():
        out.crossed()
        arrive(down.cross())
        start(written[1:4:2])
        proj.finish(FOUR)
        for item in (gate, out, down):
            item.finish()
        for copy in written:
            copy.wait()


def front(x, weights):
    heads = (HEADS, TB, HEAD)
    matrices = [(XS, YS, ROWS, QKV), (XS, YS, ROWS, WIDTH), (XS, YS, ROWS, 2 * FF), (XS, YS, DOWN, WIDTH)]
    return call(
        front_kernel, "front", TOKENS // TB,
        [(x, pl.BlockSpec(memory_space=pl.ANY)), *[(w, whole(*w.shape)) for w in weights], *tables()],
        [(low(HEADS, TOKENS, HEAD), block(*heads, dim=1)), (low(TOKENS, HEAD), block(TB, HEAD)), (low(TOKENS, HEAD), block(TB, HEAD)),
         (low(HEADS, TOKENS, HEAD), block(*heads, dim=1)), (low(HEADS, HEAD, TOKENS), block(HEADS, HEAD, TB, dim=2)), (wide(HEADS, TOKENS), block(HEADS, TB, dim=1)),
         *[(low(*s), pl.BlockSpec(memory_space=pl.ANY)) for s in ((WIDTH, TOKENS), *matrices)]],
        [VMEM(s, LOW) for s in (*matrices, (TOKENS, WIDTH), (WIDTH, TOKENS), (TOKENS, WIDTH))]
        + [VMEM((ZS, 8, n), LOW) for n in (QKV // 2, WIDTH // 2, FF)]
        + [VMEM((ROWS, FF), WIDE), VMEM((TOKENS, HEAD), LOW), VMEM((TOKENS, HEAD), LOW), VMEM((1, HEADS * TB), WIDE), VMEM((HEAD + 8, HEADS * TB), WIDE),
           VMEM((BK, STRIP), jnp.int32), DMA((6,))]
        + pairs((3, 7), (3, 2, 4), (3, 2, 4), (3, 2, 4), (4,), (4,), (8,), (1,)),
        2 * TOKENS * (WIDTH * QKV + HEADS * TOKENS * HEAD), 0)


def mlp_kernel(x_first, o_first, x_next, o_next, dy, o_last, dy_last, wo, ot_in, gu_in, wd_in, act, by_gu, bt, by_h, by_o, delta, dwo,
               h_s, scale_s, b_s, by_b_s, dh_s, ot, gu, wd, here):
    i = pl.program_id(0)
    steps = TOKENS // TB
    every, dh_s = dh_s, dh_s.at[tile(jnp.maximum(i - 1, 0), TB)]

    def first(x, o, n):
        heads = jnp.concatenate([o[h] for h in range(HEADS)], axis=1)
        h = (x[:].astype(WIDE) + mm(heads, wo[:]).astype(LOW).astype(WIDE)).astype(LOW)
        _, scale, b = scaled(h)
        h_s[n % 3] = h
        scale_s[n % 3] = scale
        b_s[n % 2] = b

    def norm_back():
        n = (i + 2) % 3
        dh = (dy_last[:].astype(WIDE) + unscaled(by_b_s[:], h_s[n].astype(WIDE), scale_s[n])).astype(LOW)
        by_h[:] = dh
        dh_s[:] = dh

    def out_back():
        do = mm_t(dh_s[:], wo[:]).astype(LOW)
        for n in range(HEADS):
            piece = do[:, n * HEAD : n * HEAD + HEAD]
            by_o[n] = piece
            delta[n : n + 1, :] = (piece.astype(WIDE) * o_last[n].astype(WIDE)).T.sum(axis=0, keepdims=True)

    loads = [pltpu.make_async_copy(src, dst, here.at[n]) for n, (src, dst) in enumerate(((gu_in, gu), (wd_in, wd), (ot_in, ot)))]

    @on(0)
    def _():
        start(loads[:2])
        first(x_first, o_first, 0)
        for load in loads[:2]:
            load.wait()

    @on(1)
    def _():
        start(loads[2:])

    @pl.when(i < steps)
    def _():
        b, dy_b = b_s[i % 2], dy[:]
        step = 1024

        def products(s):
            return mm(b, gu[:, s : s + step]), mm(b, gu[:, FF + s : FF + s + step]), mm_t(dy_b, wd[s : s + step, :]).astype(LOW)

        def between(s, g, u, by):
            f, f_up = slice(s, s + step), slice(FF + s, FF + s + step)
            by = by.astype(WIDE)
            sig = 0.5 * jnp.tanh(0.5 * g) + 0.5
            silu = g * sig
            act[:, f] = (silu * u).astype(LOW)
            by_gu[:, f_up] = (by * silu).astype(LOW)
            by_gu[:, f] = (by * u * (sig + silu * (1.0 - sig))).astype(LOW)

        made = products(0)
        norm_back()
        coming = products(step)
        between(0, *made)
        out_back()
        first(x_next, o_next, i + 1)
        between(step, *coming)
        bt[:] = b.T
        by_b_s[:] = mm_t(by_gu[:], gu[:])

    @on(steps)
    def _():
        norm_back()
        out_back()
        loads[2].wait()

        def rows(n, _):
            dwo[tile(n, SUB), :] = mm(ot[tile(n, SUB), :], every[:]).astype(LOW)

        lax.fori_loop(0, KEYS // SUB, rows, None)


def mlp(x, dy, o, ot, wo, gu, wd):
    steps = TOKENS // TB
    now, after, before = (lambda i: jnp.minimum(i, steps - 1)), (lambda i: jnp.minimum(i + 1, steps - 1)), (lambda i: jnp.maximum(i - 1, 0))
    rows = lambda at: block(TB, WIDTH, at=at)
    heads = lambda at: block(HEADS, TB, HEAD, at=at, dim=1)
    ff = lambda n: block(TB, n, at=now)
    held = ot.reshape(KEYS, TOKENS), gu, wd
    return call(
        mlp_kernel, "mlp", steps + 1,
        [(x, whole(TB, WIDTH)), (o, whole(HEADS, TB, HEAD)), (x, rows(after)), (o, heads(after)), (dy, rows(now)), (o, heads(before)), (dy, rows(before)),
         (wo, whole(KEYS, WIDTH)), *[(a, pl.BlockSpec(memory_space=pl.ANY)) for a in held]],
        [(low(TOKENS, FF), ff(FF)), (low(TOKENS, 2 * FF), ff(2 * FF)), (low(WIDTH, TOKENS), block(WIDTH, TB, at=now, dim=1)), (low(TOKENS, WIDTH), rows(before)),
         (low(HEADS, TOKENS, HEAD), heads(before)), (wide(HEADS, TOKENS), block(HEADS, TB, at=before, dim=1)), (low(KEYS, WIDTH), whole(KEYS, WIDTH))],
        [VMEM((3, TB, WIDTH), LOW), VMEM((3, TB, 1), WIDE), VMEM((2, TB, WIDTH), LOW), VMEM((TB, WIDTH), WIDE), VMEM((TOKENS, WIDTH), LOW),
         *[VMEM(a.shape, LOW) for a in held], DMA((3,))],
        2 * TOKENS * WIDTH * (3 * WIDTH + 5 * FF))


CHUNKS = FF // CHUNK
BY_Z = 512


def back_kernel(bt, dy, act, by_gate, by_up, dwo, q, k, v, do, lse, delta, dq, dk, dv, sum_o, sum_g, sum_u, sum_d, sum_z,
                dg_s, du_s, dd_s, dq_s, dk_s, dv_s, gap_s, *rest):
    i = pl.program_id(0)
    cols = HEADS * BQ
    strips = range(0, cols, STRIP)
    sems = paired(rest[15:])
    more = slice(BY_Z, WIDTH)
    of = lambda n: rest[3 * n : 3 * n + 3]
    gate = Scatter(0, True, lambda s, to: dg_s.at[s, to], sum_g, of(0), sems)
    up = Scatter(1, False, lambda s, to: du_s.at[s, :, to], sum_u, of(1), sems)
    out = Scatter(2, True, lambda s, to: dwo.at[to], sum_o, of(2), sems)
    down = Scatter(3, False, lambda s, to: dd_s.at[:, to, :, more], sum_d, of(3), sems)
    down_z = ScatterZ(dd_s, sum_z, of(4), sems[2:])

    @on(0)
    def _():
        place_ = lax.broadcasted_iota(jnp.int32, (BQ, STRIP), 1)
        gap_s[:] = jnp.where(place_ >= BQ, place_ - BQ, place_) - lax.broadcasted_iota(jnp.int32, (BQ, STRIP), 0)
        dk_s[:] = jnp.zeros_like(dk_s)
        dv_s[:] = jnp.zeros_like(dv_s)
        greet(False)

    @on(1)
    def _():
        met(False)
        start(out.first(0))

    @pl.when((i > 0) & (i <= CHUNKS))
    def _():
        start(down_z.first(i - 1) + gate.first(i - 1) + up.first(i - 1))

    @pl.when(i < CHUNKS)
    def _():
        dd_s[i // 2, pl.ds(i % 2 * 2, 2)] = t_mm(act[:], dy[:]).astype(LOW).reshape(2, DOWN, WIDTH)
        dg_s[i] = mm(bt[:], by_gate[:]).astype(LOW).reshape(XS, YS, ROWS, CHUNK)
        du_s[i] = mm(bt[:], by_up[:]).astype(LOW).reshape(XS, YS, ROWS, CHUNK)

    @on(CHUNKS)
    def _():
        start(down.first(0))

    @on(CHUNKS + 6)
    def _():
        for item in (out, gate, up, down, down_z):
            item.add_first()

    @pl.when(i >= CHUNKS)
    def _():
        iq = i - CHUNKS
        dq_s[:] = jnp.zeros_like(dq_s)
        lses = jnp.concatenate([lse[h : h + 1, :] for h in range(HEADS)], axis=1) * LOG2E
        deltas = jnp.concatenate([delta[h : h + 1, :] for h in range(HEADS)], axis=1)

        def keys(j, masked, size=BK):
            here = tile(j, size)
            qs = [q[:].reshape(cols, HEAD)[s : s + STRIP, :] for s in strips]
            dos = [do[:].reshape(cols, HEAD)[s : s + STRIP, :] for s in strips]
            scores = [mm_t(k[here, :], t) for t in qs]
            dps = [mm_t(v[here, :], t) for t in dos]
            kt = k[here, :].T
            ok = gap_s[:] >= 0 if masked else None
            for n, s in enumerate(strips):
                p = jnp.exp2(scores[n] * E - lses[:, s : s + STRIP])
                if masked:
                    p = jnp.where(ok, p, 0.0)
                ds = (p * (dps[n] - deltas[:, s : s + STRIP])).astype(LOW)
                dv_s[here, :] += mm(p.astype(LOW), dos[n])
                dk_s[here, :] += mm(ds, qs[n])
                dq_s[:, s : s + STRIP] += mm(kt, ds)

        full = iq * BQ // BK
        lax.fori_loop(0, full, lambda j, _: keys(j, False), None)

        @pl.when(iq % 2 == 1)
        def _():
            keys(iq - 1, False, BQ)

        keys(iq, True, BQ)
        for h in range(HEADS):
            dq[h] = (dq_s[:, h * BQ : h * BQ + BQ] * SCALE).T.astype(LOW)

    @on(CHUNKS + TOKENS // BQ - 1)
    def _():
        dk[:] = (dk_s[:] * SCALE).astype(LOW)
        dv[:] = dv_s[:].astype(LOW)

        for item in (down_z, out, gate, up, down):
            item.add_second()
            item.finish()


def back(bt, dy, act, by_gu, dwo, q, k, v, do, lse, delta):
    early, late = (lambda i: jnp.minimum(i, CHUNKS - 1)), (lambda i: jnp.maximum(i - CHUNKS, 0))
    cols = block(TOKENS, CHUNK, at=early, dim=1)
    heads, stats = block(HEADS, BQ, HEAD, at=late, dim=1), block(HEADS, BQ, at=late, dim=1)
    keys = whole(TOKENS, HEAD)
    sums = [(1, ROWS, WIDTH), (CHUNKS, ROWS, CHUNK), (CHUNKS, ROWS, CHUNK), (1, DOWN, WIDTH - BY_Z), (YS, TILE, BY_Z)]
    return call(
        back_kernel, "back", CHUNKS + TOKENS // BQ,
        [(bt, whole(WIDTH, TOKENS)), (dy, whole(TOKENS, WIDTH)), (act, cols), (by_gu, cols), (by_gu, block(TOKENS, CHUNK, at=lambda i: CHUNKS + early(i), dim=1)), (dwo, whole(*dwo.shape)),
         (q, heads), (k, keys), (v, keys), (do, heads), (lse, stats), (delta, stats)],
        [(low(HEADS, TOKENS, HEAD), heads), (low(TOKENS, HEAD), keys), (low(TOKENS, HEAD), keys), *[(wide(*s), whole(*s)) for s in sums]],
        [VMEM((CHUNKS, XS, YS, ROWS, CHUNK), LOW), VMEM((CHUNKS, XS, YS, ROWS, CHUNK), LOW), VMEM((XS, YS, DOWN, WIDTH), LOW), VMEM((HEAD, HEADS * BQ), WIDE),
         VMEM((TOKENS, HEAD), WIDE), VMEM((TOKENS, HEAD), WIDE), VMEM((BQ, STRIP), jnp.int32)]
        + Scatter.scratch(CHUNKS, ROWS, CHUNK) + Scatter.scratch(CHUNKS, ROWS, CHUNK) + Scatter.scratch(1, ROWS, WIDTH) + Scatter.scratch(1, DOWN, WIDTH - BY_Z)
        + ScatterZ.scratch(BY_Z) + pairs((4, 4), (4, 4), (7,), (4,)),
        2 * TOKENS * (WIDTH * 3 * FF + 3 * HEADS * TOKENS * HEAD), 1)


def tail_kernel(x, at_in, dh, dq, dk, dv, w, nc, ns, fc, fs, sum_o, sum_g, sum_u, sum_d, sum_z, dx, out_q, out_k, out_v, out_o, out_g, out_u, out_d,
                by_s, at_s, here, terms, own, *rest):
    i = pl.program_id(0)
    steps = TOKENS // TB
    sems = paired(rest[26:])
    of = lambda n: rest[3 * n : 3 * n + 3]
    one = Scatter(0, True, lambda s, to: terms.at[0, to], own.at[:1], of(0), sems)
    two = Scatter(1, False, lambda s, to: terms.at[1, :, to], own.at[1:], of(1), sems)
    gate, up, out, down, last_one, last_two = [Last(n, ref, of(2 + n), sems[2]) for n, ref in enumerate((sum_g, sum_u, sum_o, sum_d, own.at[:1], own.at[1:]))]
    down_z = LastY(sum_z, rest[24:26], sems[3])
    load = pltpu.make_async_copy(at_in, at_s, here.at[0])

    def put(ref, first=0):
        def store(s, value):
            ref[0, :, first + s * value.shape[1] : first + (s + 1) * value.shape[1]] = value
        return store

    @on(0)
    def _():
        greet(False)
        load.start()
        for item in (gate, up, out, down, last_one, last_two):
            item.clear()

    @pl.when(i < steps)
    def _():
        for n in range(TB // SUB):
            cos, sin = angles(nc, ns, fc, fs, i * (TB // SUB) + n)
            r = slice(n * SUB, n * SUB + SUB)
            here = pl.ds(many(i, TB) + n * SUB, SUB)
            for h in range(HEADS + 1):
                t = (dq[h, r, :] if h < HEADS else dk[r, :]).astype(WIDE)
                by_s[here, h * HEAD : h * HEAD + HEAD] = (t * cos - pltpu.roll(t, HEAD // 2, 1) * sin).astype(LOW)
        by_s[tile(i, TB), KEYS + HEAD :] = dv[:]

    @on(steps)
    def _():
        load.wait()

    @pl.when((i >= steps) & (i < steps + 2))
    def _():
        half = tile(i - steps, QKV // 2)
        total = mm(at_s[:], by_s[:, half])
        terms[i - steps] = total.astype(LOW).reshape(XS, YS, ROWS, QKV // 2)

    @on(steps)
    def _():
        met(False)
        start(one.first(0))

    @on(steps + 1)
    def _():
        start(two.first(0))
        for item in (down_z, out, gate, up, down):
            item.send()

    @on(2 * steps + 1)
    def _():
        one.add_first()
        two.add_first()

    @pl.when(i >= steps + 2)
    def _():
        mine = tile(i - steps - 2, TB)
        h, scale, _ = scaled(x[:])
        dx[:] = (dh[:].astype(WIDE) + unscaled(mm_t(by_s[mine, :], w[:]), h, scale)).astype(LOW)

    @on(2 * steps + 1)
    def _():
        down_z.receive(functools.partial(put(out_d), 0))
        out.receive(put(out_o))
        gate.receive(put(out_g))
        up.receive(put(out_u))
        down.receive(put(out_d, BY_Z))
        one.add_second()
        last_one.send()
        two.add_second()
        last_two.send()

        def store_one(s, value):
            out_q[0, :, : QKV // 2] = value

        def store_two(s, value):
            out_q[0, :, QKV // 2 :] = value[:, : KEYS - QKV // 2]
            out_k[0] = value[:, KEYS - QKV // 2 : KEYS - QKV // 2 + HEAD]
            out_v[0] = value[:, KEYS - QKV // 2 + HEAD :]

        last_one.receive(store_one)
        last_two.receive(store_two)
        one.finish()
        two.finish()


def tail(x, at, dh, dq, dk, dv, w, sums):
    steps = TOKENS // TB
    early, late = (lambda i: jnp.minimum(i, steps - 1)), (lambda i: jnp.maximum(i - steps - 2, 0))
    token = block(TB, HEAD, at=early)
    results = [(EACH, KEYS), (EACH, HEAD), (EACH, HEAD), (EACH, WIDTH), (EACH, FF), (EACH, FF), (TILE, WIDTH)]
    half = (1, ROWS, QKV // 2)
    forms = [(CHUNKS, ROWS, CHUNK), (CHUNKS, ROWS, CHUNK), (1, ROWS, WIDTH), (1, DOWN, WIDTH - BY_Z), half, half]
    return call(
        tail_kernel, "tail", 2 * steps + 2,
        [(x, block(TB, WIDTH, at=late)), (at, pl.BlockSpec(memory_space=pl.ANY)), (dh, block(TB, WIDTH, at=late)), (dq, block(HEADS, TB, HEAD, at=early, dim=1)), (dk, token), (dv, token),
         (w, whole(WIDTH, QKV)), *tables(), *[(s, whole(*s.shape)) for s in sums]],
        [(low(TOKENS, WIDTH), block(TB, WIDTH, at=late)), *[(low(1, *s), whole(1, *s)) for s in results]],
        [VMEM((TOKENS, QKV), LOW), VMEM((WIDTH, TOKENS), LOW), DMA((1,)), VMEM((2, XS, YS, ROWS, QKV // 2), LOW), VMEM((2, ROWS, QKV // 2), WIDE)]
        + [s for form in (half, half) for s in Scatter.scratch(*form)] + [s for form in forms for s in Last.scratch(*form)] + LastY.scratch(BY_Z)
        + pairs((2, 4), (2, 4), (6, 7), (4,)),
        4 * TOKENS * WIDTH * QKV, 2)


def publish_kernel(*refs):
    half = len(refs) // 2
    for src, dst in zip(refs[:half], refs[half:]):
        dst[:] = src[:]


def publish(dx, *rest):
    arrays = [(dx, block(TB, WIDTH)), *[(a, whole(*a.shape)) for a in rest]]
    return call(publish_kernel, "publish", TOKENS // TB, arrays, [(low(*a.shape), s) for a, s in arrays], [], 0)


def solution(mesh):
    def step(x, dy, *weights):
        x, dy = x[0], dy[0]
        q, k, v, o, ot, lse, at, w, wo, gu, wd = front(x, weights)
        act, by_gu, bt, dh, by_o, delta, dwo = mlp(x, dy, o, ot, wo.reshape(KEYS, WIDTH), gu.reshape(WIDTH, 2 * FF), wd.reshape(FF, WIDTH))
        dq, dk, dv, *sums = back(bt, dy, act, by_gu, dwo.reshape(XS, YS, ROWS, WIDTH), q, k, v, by_o, lse, delta)
        dx, *by_weights = publish(*tail(x, at, dh, dq, dk, dv, w.reshape(WIDTH, QKV), sums))
        return dx[None], *by_weights

    states, cut = P(("rep", "dp"), None, None), P(None, "dp", None)
    return jax.shard_map(
        step,
        mesh=mesh,
        in_specs=(states, states) + (cut,) * 7,
        out_specs=(states,) + (P("rep", "dp", None),) * 7,
        check_vma=False,
    )
```

```python
import functools

import jax
import jax.numpy as jnp
import numpy as np
from jax import lax
from jax.experimental import pallas as pl
from jax.experimental.pallas import tpu as pltpu
from jax.sharding import PartitionSpec as P

NEG = -1e30
HIDDEN = 2 * NEG
LOG2E = 1.4426950408889634
TOKENS, WIDTH, HEADS, HEAD, FF, THETA = 2048, 768, 6, 128, 2048, 10000
QKV, KEYS = 1024, HEADS * HEAD
LOW, WIDE = jnp.bfloat16, jnp.float32
TB = 512
SUB = 128
SCALE = HEAD**-0.5
E = SCALE * LOG2E
BK, STRIP = 512, 512
BQ = 256
CHUNK = 256
XS, YS, ZS = 4, 4, 8
FOUR = (1, 2, 3)
EIGHT = tuple(range(1, ZS))
ROWS = WIDTH // (XS * YS)
EACH = ROWS // ZS
TILE = 16
DOWN = FF // (XS * YS)
ALL = slice(None)
VMEM, DMA = pltpu.VMEM, pltpu.SemaphoreType.DMA


def _dot(a, b, ca, cb):
    return lax.dot_general(a, b, (((ca,), (cb,)), ((), ())), preferred_element_type=WIDE)


def mm(a, b):
    return _dot(a, b, 1, 0)


def mm_t(a, b):
    return _dot(a, b, 1, 1)


def t_mm(a, b):
    return _dot(a, b, 0, 0)


def low(*shape):
    return jax.ShapeDtypeStruct(shape, LOW)


def wide(*shape):
    return jax.ShapeDtypeStruct(shape, WIDE)


def many(n, size):
    return pl.multiple_of(n * size, size)


def tile(n, size=TILE):
    return pl.ds(many(n, size), size)


def block(*shape, at=lambda i: i, dim=0):
    return pl.BlockSpec(shape, lambda i: tuple(at(i) if n == dim else 0 for n in range(len(shape))))


def whole(*shape):
    return pl.BlockSpec(shape, lambda i: (0,) * len(shape), pipeline_mode=pl.Buffered(1))


def call(kernel, name, steps, ins, outs, scratch, flops, number=None):
    more = {} if number is None else {"collective_id": number, "has_side_effects": True}
    moved = sum(a.size * a.dtype.itemsize for a, _ in (*ins, *outs))
    return pl.pallas_call(
        kernel,
        name=name,
        grid=(steps,),
        in_specs=[s for _, s in ins],
        out_specs=[s for _, s in outs],
        out_shape=[a for a, _ in outs],
        scratch_shapes=scratch,
        compiler_params=pltpu.CompilerParams(dimension_semantics=("arbitrary",), vmem_limit_bytes=67_000_000, **more),
        cost_estimate=pl.CostEstimate(flops=flops, bytes_accessed=moved, transcendentals=0),
    )(*[a for a, _ in ins])


def on(n):
    return pl.when(pl.program_id(0) == n)


def always(f):
    f()


MESH = pl.DeviceIdType.MESH
NEAR, FAR = (1, 7, 2, 6), (3, 5, 4)
NEXT = (1, 3)


def place():
    me = lax.axis_index("dp")
    return lax.axis_index("rep"), me // (YS * ZS), (me // ZS) % YS, me % ZS


def at(x, y, z):
    return {"dp": (x * YS + y) * ZS + z}


def greet(sibling):
    c, x, y, z = place()
    devices = [at(x, y, (z + d) % ZS) for d in EIGHT] + [at(x, (y + d) % YS, z) for d in FOUR] + [at((x + d) % XS, y, z) for d in FOUR]
    devices += [{"rep": 1 - c}] if sibling else []
    barrier = pltpu.get_barrier_semaphore()
    for device in devices:
        pl.semaphore_signal(barrier, inc=1, device_id=device, device_id_type=MESH)


def met(sibling):
    pl.semaphore_wait(pltpu.get_barrier_semaphore(), len(EIGHT) + len(FOUR) + len(FOUR) + sibling)


def remote(src, dst, sems, at_sem, device):
    return pltpu.make_async_remote_copy(src_ref=src, dst_ref=dst, send_sem=sems[0].at[at_sem], recv_sem=sems[1].at[at_sem], device_id=device, device_id_type=MESH)


def start(copies):
    for copy in copies:
        copy.start()


def arrive(copies):
    for copy in copies:
        copy.wait_recv()


def leave(copies):
    for copy in copies:
        copy.wait_send()


class Gather:
    def __init__(self, number, out, buf, cut, sems):
        self.number, self.out, self.buf, self.sems = number, out, buf, sems
        self.c, self.x, self.y, self.z = place()
        self.half = out.shape[3] // 2
        self.a, self.b = (pl.ds(pl.multiple_of(self.c * self.half + s, HEAD), n) for s, n in ((0, cut), (cut, self.half - cut)))
        self.other = {"rep": 1 - self.c}

    def along_z(self):
        own = self.buf.at[self.z]
        return [remote(own, own, self.sems[0], (self.number, d - 1), at(self.x, self.y, (self.z + d) % ZS)) for d in EIGHT]

    def assemble(self, tmp):
        half = self.half
        for j in range(ZS):
            tmp[EACH * j : EACH * j + EACH, :half] = self.buf[j, :EACH, :].astype(WIDE)
        for n in range(2):
            @pl.when(self.c == n)
            def _():
                self.out[self.x, self.y, :, n * half : n * half + half] = tmp[:, :half].astype(LOW)

    def to_x(self, ref, sems, at_sem, ds=FOUR):
        return [remote(ref, ref, sems, (self.number, *at_sem, d), at((self.x + d) % XS, self.y, self.z)) for d in ds]

    def to_y(self, ref, sems, at_sem, ds=FOUR):
        return [remote(ref, ref, sems, (self.number, *at_sem, d), at(self.x, (self.y + d) % YS, self.z)) for d in ds]

    def second_a(self):
        return self.to_y(self.out.at[self.x, self.y, :, self.a], self.sems[1], (0,))

    def second_b(self):
        return self.to_x(self.out.at[self.x, self.y, :, self.b], self.sems[1], (1,))

    def third_a(self, ds=FOUR):
        return self.to_x(self.out.at[self.x, :, :, self.a], self.sems[2], (0,), ds)

    def third_b(self, ds=FOUR):
        return self.to_y(self.out.at[:, self.y, :, self.b], self.sems[2], (1,), ds)

    def relay_a(self):
        left, right = ((self.x + d) % XS for d in (3, 1))
        return [remote(ref, ref, self.sems[2], (self.number, 0, n), at(to, self.y, self.z)) for ref, n, to in (
            (self.out.at[left, :2, :, self.a], 0, right), (self.out.at[right, 2:, :, self.a], 2, left))]

    def relay_b(self):
        left, right = ((self.y + d) % YS for d in (3, 1))
        return [remote(ref, ref, self.sems[2], (self.number, 1, n), at(self.x, to, self.z)) for ref, n, to in (
            (self.out.at[:2, left, :, self.b], 0, right), (self.out.at[2:, right, :, self.b], 2, left))]

    def cross_a(self, d):
        got = self.out.at[(self.x - d + XS) % XS, :, :, self.a]
        return [remote(got, got, self.sems[3], (self.number, 0, d), self.other)]

    def cross_b(self, d):
        got = self.out.at[:, (self.y - d + YS) % YS, :, self.b]
        return [remote(got, got, self.sems[3], (self.number, 1, d), self.other)]

    def spread(self, ds=NEXT):
        arrive(self.second_a())
        start(self.third_a(ds))
        arrive(self.second_b())
        start(self.third_b(ds) + self.cross_a(0) + self.cross_b(0))

    def cross(self):
        for d in (1, 3, 2):
            arrive(self.third_a((d,)))
            start(self.cross_a(d))
            arrive(self.third_b((d,)))
            start(self.cross_b(d))

    def relay(self):
        arrive(self.third_a(NEXT))
        start(self.relay_a())
        arrive(self.third_b(NEXT))
        start(self.relay_b() + [copy for d in NEXT for copy in self.cross_a(d) + self.cross_b(d)])

    def relayed(self):
        arrive(self.relay_a())
        start(self.cross_a(2))
        arrive(self.relay_b())
        start(self.cross_b(2))

    def crossed(self):
        for d in range(XS):
            arrive(self.cross_a(d) + self.cross_b(d))

    def finish(self, ds=NEXT):
        leave(self.along_z() + self.second_a() + self.second_b() + self.third_a(ds) + self.third_b(ds))
        if ds == NEXT:
            leave(self.relay_a() + self.relay_b())
        for d in range(XS):
            leave(self.cross_a(d) + self.cross_b(d))


class GatherZ:
    def __init__(self, out, sems):
        self.out, self.sems = out, sems
        self.c, self.x, self.y, self.z = place()
        self.half = out.shape[3] // 2
        self.cols = pl.ds(pl.multiple_of(self.c * self.half, HEAD), self.half)

    def first(self):
        own = self.out.at[self.x, self.y, tile(self.z), self.cols]
        return [remote(own, own, self.sems[0], d, at((self.x + d) % XS, self.y, self.z)) for d in FOUR]

    def second(self):
        own = self.out.at[:, self.y, tile(self.z), self.cols]
        return [remote(own, own, self.sems[1], d, at(self.x, (self.y + d) % YS, self.z)) for d in FOUR]

    def third(self, ds):
        own = self.out.at[:, :, tile(self.z), self.cols]
        return [remote(own, own, self.sems[2], d, at(self.x, self.y, (self.z + d) % ZS)) for d in ds]

    def cross(self, ds):
        got = [self.out.at[:, :, tile((self.z - d + ZS) % ZS), self.cols] for d in ds]
        return [remote(ref, ref, self.sems[3], d, {"rep": 1 - self.c}) for d, ref in zip(ds, got)]

    def finish(self):
        leave(self.first() + self.second() + self.third(NEAR + FAR) + self.cross(range(ZS)))


class Scatter:
    @staticmethod
    def scratch(chunks, rows, cols):
        return [VMEM((3, chunks, 4, rows, cols), LOW), VMEM((4, chunks, rows, cols), LOW), VMEM((3, chunks, rows, cols), LOW)]

    def __init__(self, number, x_first, term, own, bufs, sems):
        self.number, self.term, self.own, self.sems = number, term, own, sems
        self.got, self.part, self.got2 = bufs
        c, x, y, self.z = place()
        self.p, self.q = (x, y) if x_first else (y, x)
        self.chip = (lambda p, q, z: at(p, q, z)) if x_first else (lambda p, q, z: at(q, p, z))
        self.chunks, self.rows, cols = own.shape
        self.step = {ROWS: ROWS, DOWN: DOWN // 2}[self.rows] if cols <= CHUNK else TILE

    def first(self, s):
        return [remote(self.term(s, (self.p + d) % 4), self.got.at[d - 1, s], self.sems[0], (self.number, d), self.chip((self.p + d) % 4, self.q, self.z)) for d in FOUR]

    def first_all(self):
        return [remote(self.got.at[d - 1], self.got.at[d - 1], self.sems[0], (self.number, d), self.chip((self.p + d) % 4, self.q, self.z)) for d in FOUR]

    def second(self):
        return [remote(self.part.at[(self.q + d) % 4], self.got2.at[d - 1], self.sems[1], (self.number, d), self.chip(self.p, (self.q + d) % 4, self.z)) for d in FOUR]

    def add_first(self):
        arrive(self.first_all())
        per = self.rows // self.step

        def total(s, b, r):
            total = self.term(s, self.p)[b, r, :].astype(WIDE)
            for d in FOUR:
                total += self.got[d - 1, s, b, r, :].astype(WIDE)
            return total

        def add(k, _):
            s, b, r = k // (3 * per), (self.q + 1 + k // per % 3) % 4, tile(k % per, self.step)
            self.part[b, s, r, :] = total(s, b, r).astype(LOW)

        lax.fori_loop(0, self.chunks * 3 * per, add, None, unroll=2)
        start(self.second())

        def keep(k, _):
            s, r = k // per, tile(k % per, self.step)
            self.own[s, r, :] = total(s, self.q, r)

        lax.fori_loop(0, self.chunks * per, keep, None)

    def add_second(self):
        arrive(self.second())
        per = self.rows // self.step

        def add(k, _):
            s, r = k // per, tile(k % per, self.step)
            total = self.own[s, r, :]
            for d in FOUR:
                total += self.got2[d - 1, s, r, :].astype(WIDE)
            self.own[s, r, :] = total

        lax.fori_loop(0, self.chunks * per, add, None)

    def finish(self):
        leave(self.first_all() + self.second())


class Last:
    @staticmethod
    def scratch(chunks, rows, cols):
        each = max(rows // ZS, 8)
        return [VMEM((ZS, chunks, each, cols), LOW), VMEM((ZS - 1, chunks, each, cols), LOW), VMEM((chunks, each, cols), WIDE)]

    def __init__(self, number, sums, bufs, sems):
        self.number, self.sums, self.sems = number, sums, sems
        self.packed, self.got, self.own = bufs
        self.chunks, rows, _ = sums.shape
        self.each = rows // ZS
        c, self.x, self.y, self.z = place()

    def clear(self):
        if self.each < 8:
            self.packed[:] = jnp.zeros_like(self.packed)

    def copies(self):
        return [remote(self.packed.at[(self.z + d) % ZS], self.got.at[d - 1], self.sems, (self.number, d - 1), at(self.x, self.y, (self.z + d) % ZS)) for d in EIGHT]

    def send(self):
        each = self.each

        def pack(s, _):
            for j in range(ZS):
                self.packed[j, s, :each, :] = self.sums[s, j * each : j * each + each, :].astype(LOW)

        lax.fori_loop(0, self.chunks, pack, None)
        start(self.copies())
        for j in range(ZS):
            @pl.when(self.z == j)
            def _():
                for s in range(self.chunks):
                    self.own[s, :each, :] = self.sums[s, j * each : j * each + each, :]

    def receive(self, store):
        arrive(self.copies())
        for s in range(self.chunks):
            total = self.own[s, : self.each, :]
            for d in EIGHT:
                total += self.got[d - 1, s, : self.each, :].astype(WIDE)
            store(s, total.astype(LOW))
        leave(self.copies())


class ScatterZ:
    @staticmethod
    def scratch(cols):
        return [VMEM((ZS - 1, XS, YS, TILE, cols), LOW), VMEM((XS, YS, TILE, cols), LOW), VMEM((3, YS, TILE, cols), LOW)]

    def __init__(self, terms, own, bufs, sems):
        self.terms, self.own, self.sems = terms, own, sems
        self.got, self.part, self.got2 = bufs
        c, self.x, self.y, self.z = place()
        self.cols = pl.ds(0, self.got.shape[4])

    def first(self, s):
        x, y = s // 2, pl.ds(s % 2 * 2, 2)
        return [remote(self.terms.at[x, y, tile((self.z + d) % ZS), self.cols], self.got.at[d - 1, x, y], self.sems[0], d - 1, at(self.x, self.y, (self.z + d) % ZS)) for d in EIGHT]

    def first_all(self):
        return [remote(self.got.at[d - 1], self.got.at[d - 1], self.sems[0], d - 1, at(self.x, self.y, (self.z + d) % ZS)) for d in EIGHT]

    def second(self):
        return [remote(self.part.at[(self.x + d) % XS], self.got2.at[d - 1], self.sems[1], d, at((self.x + d) % XS, self.y, self.z)) for d in FOUR]

    def add_first(self):
        arrive(self.first_all())

        def total(x, y):
            total = self.terms[x, y, tile(self.z), self.cols].astype(WIDE)
            for d in EIGHT:
                total += self.got[d - 1, x, y].astype(WIDE)
            return total

        def add(k, _):
            x, y = (self.x + 1 + k // YS) % XS, k % YS
            self.part[x, y] = total(x, y).astype(LOW)

        lax.fori_loop(0, len(FOUR) * YS, add, None, unroll=2)
        start(self.second())

        def keep(y, _):
            self.own[y] = total(self.x, y)

        lax.fori_loop(0, YS, keep, None)

    def add_second(self):
        arrive(self.second())

        def add(y, _):
            total = self.own[y]
            for d in FOUR:
                total += self.got2[d - 1, y].astype(WIDE)
            self.own[y] = total

        lax.fori_loop(0, YS, add, None)

    def finish(self):
        leave(self.first_all() + self.second())


class LastY:
    @staticmethod
    def scratch(cols):
        return [VMEM((YS, TILE, cols), LOW), VMEM((3, TILE, cols), LOW)]

    def __init__(self, sums, bufs, sems):
        self.sums, self.sems = sums, sems
        self.packed, self.got = bufs
        c, self.x, self.y, self.z = place()

    def copies(self):
        return [remote(self.packed.at[(self.y + d) % YS], self.got.at[d - 1], self.sems, d, at(self.x, (self.y + d) % YS, self.z)) for d in FOUR]

    def send(self):
        self.packed[:] = self.sums[:].astype(LOW)
        start(self.copies())

    def receive(self, store):
        arrive(self.copies())
        total = self.sums[self.y]
        for d in FOUR:
            total += self.got[d - 1].astype(WIDE)
        store(total.astype(LOW))
        leave(self.copies())


def pairs(*shapes):
    return [DMA(s) for s in shapes for _ in range(2)]


def paired(refs):
    return [refs[n : n + 2] for n in range(0, len(refs), 2)]


def tables():
    rate = float(THETA) ** (-np.arange(HEAD // 2, dtype=np.float64) / (HEAD // 2))
    rate = np.concatenate([rate, rate])
    near, far = (np.arange(0, n, s)[:, None] * rate for n, s in ((SUB, 1), (TOKENS, SUB)))
    arrays = [jnp.asarray(f(t).reshape(s), WIDE) for t, s in ((near, near.shape), (far, (TOKENS // SUB, 1, HEAD))) for f in (np.cos, np.sin)]
    return [(a, whole(*a.shape)) for a in arrays]


def angles(near_cos, near_sin, far_cos, far_sin, n):
    nc, ns, fc, fs = near_cos[:], near_sin[:], far_cos[n], far_sin[n]
    sign = jnp.where(lax.broadcasted_iota(jnp.int32, (1, HEAD), 1) < HEAD // 2, -1.0, 1.0)
    return fc * nc - fs * ns, (fs * nc + fc * ns) * sign


def scaled(h):
    h = h.astype(WIDE)
    scale = lax.rsqrt(jnp.mean(h * h, -1, keepdims=True) + 1e-6)
    return h, scale, (h * scale).astype(LOW)


def unscaled(by, h, scale):
    by = by.astype(LOW).astype(WIDE)
    return (by * scale - h * (scale * scale * scale * jnp.mean(by * h, -1, keepdims=True))).astype(LOW).astype(WIDE)


def front_kernel(x_in, wq, wk, wv, wo, wg, wu, wd, nc, ns, fc, fs, q, k, v, o, ot, lse, at_out, q_out, o_out, g_out, d_out,
                 q_w, o_w, g_w, d_w, a_s, at_s, x, q_z, o_z, g_z, tmp, k_s, v_s, top_s, mix_s, gap_s, done, *sems):
    i = pl.program_id(0)
    cols = HEADS * TB
    strips = range(0, cols, STRIP)
    sems = paired(sems)
    written = [pltpu.make_async_copy(src, dst, done.at[n]) for n, (src, dst) in enumerate(((q_w, q_out), (o_w, o_out), (g_w, g_out), (d_w, d_out), (at_s, at_out)))]
    load = pltpu.make_async_copy(x_in, x, done.at[len(written)])
    proj, out, gate = [Gather(n, *args, sems) for n, args in enumerate(((q_w, q_z, 256), (o_w, o_z, 256), (g_w, g_z, FF // 2)))]
    down = GatherZ(d_w, sems[4:])

    @on(0)
    def _():
        greet(True)
        load.start()
        c, x_, y_, z_ = place()
        rest = (gate, out)

        @pl.when(c == 0)
        def _():
            q_z[z_, :EACH, :] = wq[0, :, : QKV // 2]

        @pl.when(c == 1)
        def _():
            q_z[z_, :EACH, : KEYS - QKV // 2] = wq[0, :, QKV // 2 :]
            q_z[z_, :EACH, KEYS - QKV // 2 : KEYS - QKV // 2 + HEAD] = wk[0]
            q_z[z_, :EACH, KEYS - QKV // 2 + HEAD :] = wv[0]

        for buf in (q_z, o_z, g_z):
            buf[z_, EACH:, :] = jnp.zeros((buf.shape[1] - EACH, buf.shape[2]), LOW)
        met(True)
        start(proj.along_z())
        for n, w in enumerate((wg, wu)):
            @pl.when(c == n)
            def _():
                g_z[z_, :EACH, :] = w[0]
                o_z[z_, :EACH, :] = wo[0, :, n * out.half : n * out.half + out.half]
                d_w[x_, y_, tile(z_), n * down.half : n * down.half + down.half] = wd[0, :, n * down.half : n * down.half + down.half]
        start(down.first())
        for item in rest:
            start(item.along_z())
        gap_s[:] = lax.broadcasted_iota(jnp.int32, (BK, STRIP), 1) - lax.broadcasted_iota(jnp.int32, (BK, STRIP), 0)

        def norm(n, _):
            a = scaled(x[tile(n, TB), :])[2]
            a_s[tile(n, TB), :] = a
            at_s[:, tile(n, TB)] = a.T

        load.wait()
        lax.fori_loop(0, TOKENS // TB, norm, None)
        start(written[4:])
        arrive(proj.along_z())
        proj.assemble(tmp)
        start(proj.second_a() + proj.second_b())
        arrive(down.first())
        start(down.second())
        proj.spread(FOUR)
        arrive(down.second())
        start(down.third(NEAR + FAR))
        for item in rest:
            arrive(item.along_z())
            item.assemble(tmp)
            start(item.second_a() + item.second_b())
        proj.cross()
        proj.crossed()
        start(written[:1])

    mine = tile(i, TB)
    made = mm(a_s[mine, :], q_w[:].reshape(WIDTH, QKV))
    for n in range(TB // SUB):
        cos, sin = angles(nc, ns, fc, fs, i * (TB // SUB) + n)
        r = slice(n * SUB, n * SUB + SUB)
        for h in range(HEADS + 1):
            t = made[r, h * HEAD : h * HEAD + HEAD].astype(LOW).astype(WIDE)
            t = (t * cos + pltpu.roll(t, HEAD // 2, 1) * sin).astype(LOW)
            if h < HEADS:
                q[h, r, :] = t
            else:
                k[r, :] = t
    v[:] = made[:, KEYS + HEAD :].astype(LOW)
    k_s[mine, :] = k[:]
    v_s[mine, :] = v[:]

    @on(0)
    def _():
        gate.spread()

    top_s[:] = jnp.full((1, cols), NEG, WIDE)
    mix_s[:] = jnp.zeros((HEAD + 8, cols), WIDE)

    def keys(j, size=BK, first=0, masked=False):
        here = pl.ds(many(j, BK) + first, size)
        wide_ = STRIP - first
        spans = [slice(s + first, s + STRIP) for s in strips]
        scores = [mm_t(k_s[here, :], q[:].reshape(cols, HEAD)[span, :]) for span in spans]
        ok = gap_s[:size, :wide_] >= 0 if masked else None
        weights, keeps = [], []
        for span, score in zip(spans, scores):
            if masked:
                score = jnp.where(ok, score, HIDDEN)
            old = top_s[:, span]
            top = jnp.maximum(old, score.max(axis=0, keepdims=True))
            top_s[:, span] = top
            weights.append(jnp.exp2((score - top) * E).astype(LOW))
            keeps.append(jnp.exp2((old - top) * E))
        values = jnp.concatenate([v_s[here, :].T, jnp.ones((8, size), LOW)], axis=0)
        for span, p, keep in zip(spans, weights, keeps):
            mix_s[:, span] = mix_s[:, span] * keep + mm(values, p)

    lax.fori_loop(0, i, lambda j, _: keys(j), None)

    @on(2)
    def _():
        out.relay()

    @on(3)
    def _():
        gate.crossed()
        start(written[2:3])
        out.relayed()
        arrive(down.third(NEAR))
        start(down.cross((0, *NEAR)))

    for first in (0, BK // 2):
        keys(i, BK // 2, first, True)
    total = mix_s[HEAD : HEAD + 1, :]
    result = mix_s[:HEAD, :] * (1 / total)
    lses = top_s[:] * SCALE + jnp.log(total)
    for h in range(HEADS):
        piece = result[:, h * TB : h * TB + TB].astype(LOW)
        ot[h] = piece
        o[h] = piece.T
        lse[h : h + 1, :] = lses[:, h * TB : h * TB + TB]

    @on(0)
    def _():
        out.spread()

    @on(1)
    def _():
        gate.relay()

    @on(2)
    def _():
        gate.relayed()

    @on(3)
    def _():
        arrive(down.third(FAR))
        start(down.cross(FAR))
        out.crossed()
        arrive(down.cross((0, *NEAR, *FAR)))
        start(written[1:4:2])
        proj.finish(FOUR)
        for item in (gate, out, down):
            item.finish()
        for copy in written:
            copy.wait()


def front(x, weights):
    heads = (HEADS, TB, HEAD)
    matrices = [(XS, YS, ROWS, QKV), (XS, YS, ROWS, WIDTH), (XS, YS, ROWS, 2 * FF), (XS, YS, DOWN, WIDTH)]
    return call(
        front_kernel, "front", TOKENS // TB,
        [(x, pl.BlockSpec(memory_space=pl.ANY)), *[(w, whole(*w.shape)) for w in weights], *tables()],
        [(low(HEADS, TOKENS, HEAD), block(*heads, dim=1)), (low(TOKENS, HEAD), block(TB, HEAD)), (low(TOKENS, HEAD), block(TB, HEAD)),
         (low(HEADS, TOKENS, HEAD), block(*heads, dim=1)), (low(HEADS, HEAD, TOKENS), block(HEADS, HEAD, TB, dim=2)), (wide(HEADS, TOKENS), block(HEADS, TB, dim=1)),
         *[(low(*s), pl.BlockSpec(memory_space=pl.ANY)) for s in ((WIDTH, TOKENS), *matrices)]],
        [VMEM(s, LOW) for s in (*matrices, (TOKENS, WIDTH), (WIDTH, TOKENS), (TOKENS, WIDTH))]
        + [VMEM((ZS, 8, n), LOW) for n in (QKV // 2, WIDTH // 2, FF)]
        + [VMEM((ROWS, FF), WIDE), VMEM((TOKENS, HEAD), LOW), VMEM((TOKENS, HEAD), LOW), VMEM((1, HEADS * TB), WIDE), VMEM((HEAD + 8, HEADS * TB), WIDE),
           VMEM((BK, STRIP), jnp.int32), DMA((6,))]
        + pairs((3, 7), (3, 2, 4), (3, 2, 4), (3, 2, 4), (4,), (4,), (8,), (8,)),
        2 * TOKENS * (WIDTH * QKV + HEADS * TOKENS * HEAD), 0)


def mlp_kernel(x_first, o_first, x_next, o_next, dy, o_last, dy_last, wo, ot_in, gu_in, wd_in, act, by_gu, bt, by_h, by_o, delta, dwo,
               h_s, scale_s, b_s, by_b_s, dh_s, ot, gu, wd, here):
    i = pl.program_id(0)
    steps = TOKENS // TB
    every, dh_s = dh_s, dh_s.at[tile(jnp.maximum(i - 1, 0), TB)]

    def first(x, o, n):
        heads = jnp.concatenate([o[h] for h in range(HEADS)], axis=1)
        h = (x[:].astype(WIDE) + mm(heads, wo[:]).astype(LOW).astype(WIDE)).astype(LOW)
        _, scale, b = scaled(h)
        h_s[n % 3] = h
        scale_s[n % 3] = scale
        b_s[n % 2] = b

    def norm_back():
        n = (i + 2) % 3
        dh = (dy_last[:].astype(WIDE) + unscaled(by_b_s[:], h_s[n].astype(WIDE), scale_s[n])).astype(LOW)
        by_h[:] = dh
        dh_s[:] = dh

    def out_back():
        do = mm_t(dh_s[:], wo[:]).astype(LOW)
        for n in range(HEADS):
            piece = do[:, n * HEAD : n * HEAD + HEAD]
            by_o[n] = piece
            delta[n : n + 1, :] = (piece.astype(WIDE) * o_last[n].astype(WIDE)).T.sum(axis=0, keepdims=True)

    loads = [pltpu.make_async_copy(src, dst, here.at[n]) for n, (src, dst) in enumerate(((gu_in, gu), (wd_in, wd), (ot_in, ot)))]

    @on(0)
    def _():
        start(loads[:2])
        first(x_first, o_first, 0)
        for load in loads[:2]:
            load.wait()

    @on(1)
    def _():
        start(loads[2:])

    @pl.when(i < steps)
    def _():
        b, dy_b = b_s[i % 2], dy[:]
        step = 1024

        def products(s):
            return mm(b, gu[:, s : s + step]), mm(b, gu[:, FF + s : FF + s + step]), mm_t(dy_b, wd[s : s + step, :]).astype(LOW)

        def between(s, g, u, by):
            f, f_up = slice(s, s + step), slice(FF + s, FF + s + step)
            by = by.astype(WIDE)
            sig = 0.5 * jnp.tanh(0.5 * g) + 0.5
            silu = g * sig
            act[:, f] = (silu * u).astype(LOW)
            by_gu[:, f_up] = (by * silu).astype(LOW)
            by_gu[:, f] = (by * u * (sig + silu * (1.0 - sig))).astype(LOW)

        made = products(0)
        norm_back()
        coming = products(step)
        between(0, *made)
        out_back()
        first(x_next, o_next, i + 1)
        between(step, *coming)
        bt[:] = b.T
        by_b_s[:] = mm_t(by_gu[:], gu[:])

    @on(steps)
    def _():
        norm_back()
        out_back()
        loads[2].wait()

        def rows(n, _):
            dwo[tile(n, CHUNK), :] = mm(ot[tile(n, CHUNK), :], every[:]).astype(LOW)

        lax.fori_loop(0, KEYS // CHUNK, rows, None)


def mlp(x, dy, o, ot, wo, gu, wd):
    steps = TOKENS // TB
    now, after, before = (lambda i: jnp.minimum(i, steps - 1)), (lambda i: jnp.minimum(i + 1, steps - 1)), (lambda i: jnp.maximum(i - 1, 0))
    rows = lambda at: block(TB, WIDTH, at=at)
    heads = lambda at: block(HEADS, TB, HEAD, at=at, dim=1)
    ff = lambda n: block(TB, n, at=now)
    held = ot.reshape(KEYS, TOKENS), gu, wd
    return call(
        mlp_kernel, "mlp", steps + 1,
        [(x, whole(TB, WIDTH)), (o, whole(HEADS, TB, HEAD)), (x, rows(after)), (o, heads(after)), (dy, rows(now)), (o, heads(before)), (dy, rows(before)),
         (wo, whole(KEYS, WIDTH)), *[(a, pl.BlockSpec(memory_space=pl.ANY)) for a in held]],
        [(low(TOKENS, FF), ff(FF)), (low(TOKENS, 2 * FF), ff(2 * FF)), (low(WIDTH, TOKENS), block(WIDTH, TB, at=now, dim=1)), (low(TOKENS, WIDTH), rows(before)),
         (low(HEADS, TOKENS, HEAD), heads(before)), (wide(HEADS, TOKENS), block(HEADS, TB, at=before, dim=1)), (low(KEYS, WIDTH), whole(KEYS, WIDTH))],
        [VMEM((3, TB, WIDTH), LOW), VMEM((3, TB, 1), WIDE), VMEM((2, TB, WIDTH), LOW), VMEM((TB, WIDTH), WIDE), VMEM((TOKENS, WIDTH), LOW),
         *[VMEM(a.shape, LOW) for a in held], DMA((3,))],
        2 * TOKENS * WIDTH * (3 * WIDTH + 5 * FF))


CHUNKS = FF // CHUNK
BY_Z = 512


def back_kernel(bt, dy, act, by_gate, by_up, dwo, q, k, v, do, lse, delta, dq, dk, dv, sum_o, sum_g, sum_u, sum_d, sum_z,
                dg_s, du_s, dd_s, dq_s, dk_s, dv_s, gap_s, *rest):
    i = pl.program_id(0)
    cols = HEADS * BQ
    strips = range(0, cols, STRIP)
    sems = paired(rest[15:])
    more = slice(BY_Z, WIDTH)
    of = lambda n: rest[3 * n : 3 * n + 3]
    gate = Scatter(0, True, lambda s, to: dg_s.at[s, to], sum_g, of(0), sems)
    up = Scatter(1, False, lambda s, to: du_s.at[s, :, to], sum_u, of(1), sems)
    out = Scatter(2, True, lambda s, to: dwo.at[to], sum_o, of(2), sems)
    down = Scatter(3, False, lambda s, to: dd_s.at[:, to, :, more], sum_d, of(3), sems)
    down_z = ScatterZ(dd_s, sum_z, of(4), sems[2:])

    @on(0)
    def _():
        place_ = lax.broadcasted_iota(jnp.int32, (BQ, STRIP), 1)
        gap_s[:] = jnp.where(place_ >= BQ, place_ - BQ, place_) - lax.broadcasted_iota(jnp.int32, (BQ, STRIP), 0)
        dk_s[:] = jnp.zeros_like(dk_s)
        dv_s[:] = jnp.zeros_like(dv_s)
        greet(False)

    @on(1)
    def _():
        met(False)
        start(out.first(0))

    @pl.when((i > 0) & (i <= CHUNKS))
    def _():
        start(down_z.first(i - 1) + gate.first(i - 1) + up.first(i - 1))

    @pl.when(i < CHUNKS)
    def _():
        dd_s[i // 2, pl.ds(i % 2 * 2, 2)] = t_mm(act[:], dy[:]).astype(LOW).reshape(2, DOWN, WIDTH)
        dg_s[i] = mm(bt[:], by_gate[:]).astype(LOW).reshape(XS, YS, ROWS, CHUNK)
        du_s[i] = mm(bt[:], by_up[:]).astype(LOW).reshape(XS, YS, ROWS, CHUNK)

    @on(CHUNKS)
    def _():
        start(down.first(0))

    @on(CHUNKS + 6)
    def _():
        for item in (out, gate, up, down, down_z):
            item.add_first()

    @pl.when(i >= CHUNKS)
    def _():
        iq = i - CHUNKS
        dq_s[:] = jnp.zeros_like(dq_s)
        lses = jnp.concatenate([lse[h : h + 1, :] for h in range(HEADS)], axis=1) * LOG2E
        deltas = jnp.concatenate([delta[h : h + 1, :] for h in range(HEADS)], axis=1)

        def keys(j, masked, size=BK):
            here = tile(j, size)
            qs = [q[:].reshape(cols, HEAD)[s : s + STRIP, :] for s in strips]
            dos = [do[:].reshape(cols, HEAD)[s : s + STRIP, :] for s in strips]
            scores = [mm_t(k[here, :], t) for t in qs]
            dps = [mm_t(v[here, :], t) for t in dos]
            kt = k[here, :].T
            ok = gap_s[:] >= 0 if masked else None
            for n, s in enumerate(strips):
                p = jnp.exp2(scores[n] * E - lses[:, s : s + STRIP])
                if masked:
                    p = jnp.where(ok, p, 0.0)
                ds = (p * (dps[n] - deltas[:, s : s + STRIP])).astype(LOW)
                dv_s[here, :] += mm(p.astype(LOW), dos[n])
                dk_s[here, :] += mm(ds, qs[n])
                dq_s[:, s : s + STRIP] += mm(kt, ds)

        full = iq * BQ // BK
        lax.fori_loop(0, full, lambda j, _: keys(j, False), None)

        @pl.when(iq % 2 == 1)
        def _():
            keys(iq - 1, False, BQ)

        keys(iq, True, BQ)
        for h in range(HEADS):
            dq[h] = (dq_s[:, h * BQ : h * BQ + BQ] * SCALE).T.astype(LOW)

    @on(CHUNKS + TOKENS // BQ - 1)
    def _():
        dk[:] = (dk_s[:] * SCALE).astype(LOW)
        dv[:] = dv_s[:].astype(LOW)

        for item in (down_z, out, gate, up, down):
            item.add_second()
            item.finish()


def back(bt, dy, act, by_gu, dwo, q, k, v, do, lse, delta):
    early, late = (lambda i: jnp.minimum(i, CHUNKS - 1)), (lambda i: jnp.maximum(i - CHUNKS, 0))
    cols = block(TOKENS, CHUNK, at=early, dim=1)
    heads, stats = block(HEADS, BQ, HEAD, at=late, dim=1), block(HEADS, BQ, at=late, dim=1)
    keys = whole(TOKENS, HEAD)
    sums = [(1, ROWS, WIDTH), (CHUNKS, ROWS, CHUNK), (CHUNKS, ROWS, CHUNK), (1, DOWN, WIDTH - BY_Z), (YS, TILE, BY_Z)]
    return call(
        back_kernel, "back", CHUNKS + TOKENS // BQ,
        [(bt, whole(WIDTH, TOKENS)), (dy, whole(TOKENS, WIDTH)), (act, cols), (by_gu, cols), (by_gu, block(TOKENS, CHUNK, at=lambda i: CHUNKS + early(i), dim=1)), (dwo, whole(*dwo.shape)),
         (q, heads), (k, keys), (v, keys), (do, heads), (lse, stats), (delta, stats)],
        [(low(HEADS, TOKENS, HEAD), heads), (low(TOKENS, HEAD), keys), (low(TOKENS, HEAD), keys), *[(wide(*s), whole(*s)) for s in sums]],
        [VMEM((CHUNKS, XS, YS, ROWS, CHUNK), LOW), VMEM((CHUNKS, XS, YS, ROWS, CHUNK), LOW), VMEM((XS, YS, DOWN, WIDTH), LOW), VMEM((HEAD, HEADS * BQ), WIDE),
         VMEM((TOKENS, HEAD), WIDE), VMEM((TOKENS, HEAD), WIDE), VMEM((BQ, STRIP), jnp.int32)]
        + Scatter.scratch(CHUNKS, ROWS, CHUNK) + Scatter.scratch(CHUNKS, ROWS, CHUNK) + Scatter.scratch(1, ROWS, WIDTH) + Scatter.scratch(1, DOWN, WIDTH - BY_Z)
        + ScatterZ.scratch(BY_Z) + pairs((4, 4), (4, 4), (7,), (4,)),
        2 * TOKENS * (WIDTH * 3 * FF + 3 * HEADS * TOKENS * HEAD), 1)


def tail_kernel(x, at_in, dh, dq, dk, dv, w, nc, ns, fc, fs, sum_o, sum_g, sum_u, sum_d, sum_z, dx, out_q, out_k, out_v, out_o, out_g, out_u, out_d,
                by_s, at_s, here, terms, own, *rest):
    i = pl.program_id(0)
    steps = TOKENS // TB
    sems = paired(rest[26:])
    of = lambda n: rest[3 * n : 3 * n + 3]
    one = Scatter(0, True, lambda s, to: terms.at[0, to], own.at[:1], of(0), sems)
    two = Scatter(1, False, lambda s, to: terms.at[1, :, to], own.at[1:], of(1), sems)
    gate, up, out, down, last_one, last_two = [Last(n, ref, of(2 + n), sems[2]) for n, ref in enumerate((sum_g, sum_u, sum_o, sum_d, own.at[:1], own.at[1:]))]
    down_z = LastY(sum_z, rest[24:26], sems[3])
    load = pltpu.make_async_copy(at_in, at_s, here.at[0])

    def put(ref, first=0):
        def store(s, value):
            ref[0, :, first + s * value.shape[1] : first + (s + 1) * value.shape[1]] = value
        return store

    @on(0)
    def _():
        greet(False)
        load.start()
        for item in (gate, up, out, down, last_one, last_two):
            item.clear()

    @pl.when(i < steps)
    def _():
        for n in range(TB // SUB):
            cos, sin = angles(nc, ns, fc, fs, i * (TB // SUB) + n)
            r = slice(n * SUB, n * SUB + SUB)
            here = pl.ds(many(i, TB) + n * SUB, SUB)
            for h in range(HEADS + 1):
                t = (dq[h, r, :] if h < HEADS else dk[r, :]).astype(WIDE)
                by_s[here, h * HEAD : h * HEAD + HEAD] = (t * cos - pltpu.roll(t, HEAD // 2, 1) * sin).astype(LOW)
        by_s[tile(i, TB), KEYS + HEAD :] = dv[:]

    @on(steps)
    def _():
        load.wait()

    @pl.when((i >= steps) & (i < steps + 2))
    def _():
        half = tile(i - steps, QKV // 2)
        total = mm(at_s[:], by_s[:, half])
        terms[i - steps] = total.astype(LOW).reshape(XS, YS, ROWS, QKV // 2)

    @on(steps)
    def _():
        met(False)
        start(one.first(0))

    @on(steps + 1)
    def _():
        start(two.first(0))
        for item in (down_z, out, gate, up, down):
            item.send()

    @on(2 * steps + 1)
    def _():
        one.add_first()
        two.add_first()

    @pl.when(i >= steps + 2)
    def _():
        mine = tile(i - steps - 2, TB)
        h, scale, _ = scaled(x[:])
        dx[:] = (dh[:].astype(WIDE) + unscaled(mm_t(by_s[mine, :], w[:]), h, scale)).astype(LOW)

    @on(2 * steps + 1)
    def _():
        down_z.receive(functools.partial(put(out_d), 0))
        out.receive(put(out_o))
        gate.receive(put(out_g))
        up.receive(put(out_u))
        down.receive(put(out_d, BY_Z))
        one.add_second()
        last_one.send()
        two.add_second()
        last_two.send()

        def store_one(s, value):
            out_q[0, :, : QKV // 2] = value

        def store_two(s, value):
            out_q[0, :, QKV // 2 :] = value[:, : KEYS - QKV // 2]
            out_k[0] = value[:, KEYS - QKV // 2 : KEYS - QKV // 2 + HEAD]
            out_v[0] = value[:, KEYS - QKV // 2 + HEAD :]

        last_one.receive(store_one)
        last_two.receive(store_two)
        one.finish()
        two.finish()


def tail(x, at, dh, dq, dk, dv, w, sums):
    steps = TOKENS // TB
    early, late = (lambda i: jnp.minimum(i, steps - 1)), (lambda i: jnp.maximum(i - steps - 2, 0))
    token = block(TB, HEAD, at=early)
    results = [(EACH, KEYS), (EACH, HEAD), (EACH, HEAD), (EACH, WIDTH), (EACH, FF), (EACH, FF), (TILE, WIDTH)]
    half = (1, ROWS, QKV // 2)
    forms = [(CHUNKS, ROWS, CHUNK), (CHUNKS, ROWS, CHUNK), (1, ROWS, WIDTH), (1, DOWN, WIDTH - BY_Z), half, half]
    return call(
        tail_kernel, "tail", 2 * steps + 2,
        [(x, block(TB, WIDTH, at=late)), (at, pl.BlockSpec(memory_space=pl.ANY)), (dh, block(TB, WIDTH, at=late)), (dq, block(HEADS, TB, HEAD, at=early, dim=1)), (dk, token), (dv, token),
         (w, whole(WIDTH, QKV)), *tables(), *[(s, whole(*s.shape)) for s in sums]],
        [(low(TOKENS, WIDTH), block(TB, WIDTH, at=late)), *[(low(1, *s), whole(1, *s)) for s in results]],
        [VMEM((TOKENS, QKV), LOW), VMEM((WIDTH, TOKENS), LOW), DMA((1,)), VMEM((2, XS, YS, ROWS, QKV // 2), LOW), VMEM((2, ROWS, QKV // 2), WIDE)]
        + [s for form in (half, half) for s in Scatter.scratch(*form)] + [s for form in forms for s in Last.scratch(*form)] + LastY.scratch(BY_Z)
        + pairs((2, 4), (2, 4), (6, 7), (4,)),
        4 * TOKENS * WIDTH * QKV, 2)


def publish_kernel(*refs):
    half = len(refs) // 2
    for src, dst in zip(refs[:half], refs[half:]):
        dst[:] = src[:]


def publish(dx, *rest):
    arrays = [(dx, block(TB, WIDTH)), *[(a, whole(*a.shape)) for a in rest]]
    return call(publish_kernel, "publish", TOKENS // TB, arrays, [(low(*a.shape), s) for a, s in arrays], [], 0)


def solution(mesh):
    def step(x, dy, *weights):
        x, dy = x[0], dy[0]
        q, k, v, o, ot, lse, at, w, wo, gu, wd = front(x, weights)
        act, by_gu, bt, dh, by_o, delta, dwo = mlp(x, dy, o, ot, wo.reshape(KEYS, WIDTH), gu.reshape(WIDTH, 2 * FF), wd.reshape(FF, WIDTH))
        dq, dk, dv, *sums = back(bt, dy, act, by_gu, dwo.reshape(XS, YS, ROWS, WIDTH), q, k, v, by_o, lse, delta)
        dx, *by_weights = publish(*tail(x, at, dh, dq, dk, dv, w.reshape(WIDTH, QKV), sums))
        return dx[None], *by_weights

    states, cut = P(("rep", "dp"), None, None), P(None, "dp", None)
    return jax.shard_map(
        step,
        mesh=mesh,
        in_specs=(states, states) + (cut,) * 7,
        out_specs=(states,) + (P("rep", "dp", None),) * 7,
        check_vma=False,
    )
```
